32 devices in a mesh: groups: 2 (over x), row: 16 (over z, y, core).
Axes of the slice: x: 2, y: 2, z: 4, core: 2. Of those that a mesh axis runs over, the one named last changes fastest.
Arguments:
- latent: bfloat16 [8, 16, 128, 16], P('groups', None, 'row'), parts along dimension 0, may hold values from -16 to 16, as said below
- w_in: bfloat16 [3, 3, 3, 16, 384], replicated, may hold values from -0.3125 to 0.3125
- gain_one: float32 [384], replicated, may hold values from 0.25 to 1.75
- w_mid: bfloat16 [3, 3, 3, 384, 384], replicated, may hold values from -0.0625 to 0.0625
- gain_two: float32 [384], replicated, may hold values from 0.25 to 1.75
- w_up: bfloat16 [3, 3, 384, 192], replicated, may hold values from -0.109375 to 0.109375
- gain_three: float32 [192], replicated, may hold values from 0.25 to 1.75
- w_low: bfloat16 [3, 3, 3, 192, 96], replicated, may hold values from -0.078125 to 0.078125
- gain_four: float32 [96], replicated, may hold values from 0.25 to 1.75
- w_out: bfloat16 [3, 3, 3, 96, 3], replicated, may hold values from -0.125 to 0.125
Outputs:
- frames_rgb: float32 [8, 3, 32, 256], P('groups', None, 'row'), parts along dimension 0
The draws below stay inside these ranges and needn't reach their ends.
There are 2 independent parts, one for each index of `groups`. The reference program is written for one: setup_inputs(seed, part) draws one part's arguments, and reference() takes and returns one part's arrays. A program takes and returns all parts, laid end to end along the dimension named above; an argument that names none is the same for every part. Nothing has to cross between parts.
Inputs may be any that keep to these rules, and one draw needn't show every extreme that they name: latent is real-valued.
All inputs are finite; a program needn't handle non-finite values.
Results may differ from the reference program's by a relative error of at most 0.0058.
Values may be sent and summed in bfloat16 or wider, within the bound.
A program may use at most 128 MiB of HBM per device.

```python
import math
import jax
import jax.numpy as jnp
from jax import lax

C_LAT = 16
C_HI = 384
C_MID = 192
C_LO = 96
FRAMES = 4
W = 128
H = 16


def draw_latent(key, part):
    keys = jax.random.split(jax.random.fold_in(key, 11), 5)
    shape = (FRAMES, H, W, C_LAT)
    frame_scale = jnp.exp(jax.random.uniform(keys[0], (FRAMES, 1, 1, C_LAT), jnp.float32, math.log(0.3), math.log(3.0)))
    row_scale = jnp.exp(jax.random.uniform(keys[1], (1, H, 1, 1), jnp.float32, math.log(0.4), math.log(2.5)))
    frame_shift = 0.7 * jax.random.normal(keys[2], (FRAMES, 1, 1, C_LAT), jnp.float32)
    row_shift = 0.7 * jax.random.normal(keys[3], (1, H, 1, C_LAT), jnp.float32)
    noise = jax.random.normal(keys[4], shape, jnp.float32)
    value = noise * frame_scale * row_scale + frame_shift + row_shift
    return jnp.clip(value, -16.0, 16.0).astype(jnp.bfloat16)


def scatter_about(key, shape, scale, limit, held_as=jnp.bfloat16):
    values = scale * jax.random.normal(key, shape, jnp.float32)
    return jnp.clip(values, min=-limit, max=limit).astype(held_as)


def setup_inputs(seed: int = 0, part: int = 0) -> dict:
    key_list = jax.random.split(jax.random.key(seed), 11)
    part_splits = jax.random.split(jax.random.fold_in(key_list[10], part), 11)
    latent = draw_latent(jax.random.fold_in(jax.random.fold_in(key_list[10], part), 71), part)
    w_in = scatter_about(key_list[1], (3, 3, 3, C_LAT, C_HI), (27 * C_LAT) ** -0.5, 0.3125)
    gain_one = jnp.clip(1.0 + 0.15 * jax.random.normal(key_list[2], (C_HI,), jnp.float32), 0.25, 1.75)
    w_mid = scatter_about(key_list[3], (3, 3, 3, C_HI, C_HI), (27 * C_HI) ** -0.5, 0.0625)
    gain_two = jnp.clip(1.0 + 0.15 * jax.random.normal(key_list[4], (C_HI,), jnp.float32), 0.25, 1.75)
    w_up = scatter_about(key_list[5], (3, 3, C_HI, C_MID), (9 * C_HI) ** -0.5, 0.109375)
    gain_three = jnp.clip(1.0 + 0.15 * jax.random.normal(key_list[6], (C_MID,), jnp.float32), 0.25, 1.75)
    w_low = scatter_about(key_list[7], (3, 3, 3, C_MID, C_LO), (27 * C_MID) ** -0.5, 0.078125)
    gain_four = jnp.clip(1.0 + 0.15 * jax.random.normal(key_list[8], (C_LO,), jnp.float32), 0.25, 1.75)
    w_out = scatter_about(key_list[9], (3, 3, 3, C_LO, 3), (27 * C_LO) ** -0.5, 0.125)
    return {"latent": latent, "w_in": w_in, "gain_one": gain_one, "w_mid": w_mid, "gain_two": gain_two, "w_up": w_up, "gain_three": gain_three, "w_low": w_low, "gain_four": gain_four, "w_out": w_out}


eps = 1e-06

def causal_conv(field, weight):
    frame_count, height, width, inner = field.shape
    padded = jnp.pad(field, ((2, 0), (1, 1), (1, 1), (0, 0)))
    total = jnp.zeros((frame_count * height * width, weight.shape[-1]), jnp.float32)
    for offset_t in range(3):
        for offset_h in range(3):
            for offset_w in range(3):
                window = padded[offset_t:offset_t + frame_count, offset_h:offset_h + height, offset_w:offset_w + width]
                total = total + jnp.dot(window.reshape(-1, inner), weight[offset_t, offset_h, offset_w], preferred_element_type=jnp.float32)
    return total.reshape(frame_count, height, width, -1)

def plane_conv(field, weight):
    frame_count, height, width, inner = field.shape
    padded = jnp.pad(field, ((0, 0), (1, 1), (1, 1), (0, 0)))
    total = jnp.zeros((frame_count * height * width, weight.shape[-1]), jnp.float32)
    for offset_h in range(3):
        for offset_w in range(3):
            window = padded[:, offset_h:offset_h + height, offset_w:offset_w + width]
            total = total + jnp.dot(window.reshape(-1, inner), weight[offset_h, offset_w], preferred_element_type=jnp.float32)
    return total.reshape(frame_count, height, width, -1)

def rms_act(field, gain):
    scale = lax.rsqrt(lax.optimization_barrier(jnp.mean(field * field, axis=-1, keepdims=True)) + eps)
    return jax.nn.silu(field * scale * gain).astype(jnp.bfloat16)

def reference(latent, w_in, gain_one, w_mid, gain_two, w_up, gain_three, w_low, gain_four, w_out):
    first = causal_conv(latent, w_in)
    act_one = rms_act(first, gain_one)
    second = first + causal_conv(act_one, w_mid)
    act_two = rms_act(second, gain_two)
    upsampled = jnp.repeat(jnp.repeat(act_two, 2, axis=1), 2, axis=2)
    third = plane_conv(upsampled, w_up)
    act_three = rms_act(third, gain_three)
    fourth = causal_conv(act_three, w_low)
    act_four = rms_act(fourth, gain_four)
    colour = causal_conv(act_four, w_out)
    return jnp.transpose(colour, (0, 3, 1, 2))
```

```python
import functools

import jax
import jax.numpy as jnp
from jax import lax
from jax.experimental import pallas as pl
from jax.experimental.pallas import tpu as pltpu
from jax.sharding import PartitionSpec as P

eps = 1e-06
f32, bf16, i32 = jnp.float32, jnp.bfloat16, jnp.int32
MESH = pl.DeviceIdType.MESH
LANES = 128


def half_silu(h):
    return h * jnp.tanh(h) + h


def rms_act(field, half_gain, count):
    mean = jnp.sum(field * field, axis=-1, keepdims=True) * (1.0 / count)
    return half_silu(field * lax.rsqrt(mean + eps) * half_gain)


def pair_norm(field, half_gain, low):
    half = field.shape[-1] // 2
    square = field * field
    first = jnp.sum(jnp.where(low, square, 0.0), axis=-1, keepdims=True)
    second = jnp.sum(jnp.where(low, 0.0, square), axis=-1, keepdims=True)
    inv = 1.0 / half
    scale = jnp.where(low, lax.rsqrt(first * inv + eps), lax.rsqrt(second * inv + eps))
    return half_silu(field * scale * half_gain)


def dot(a, b):
    return jnp.dot(a, b, preferred_element_type=f32)


def iota(shape, axis):
    return lax.broadcasted_iota(i32, shape, axis)


def merge(value):
    return value.reshape(-1, value.shape[-1])


def rows_of(value, count):
    return value.reshape(count, value.shape[0] // count, value.shape[1])


def kernel(
    sizes, devices, packed,
    lat_hbm, g1_ref, g2_ref, g3_ref, g4_ref,
    win_hbm, wmid_hbm, wup_hbm, wlow_hbm, wout_hbm,
    out_ref,
    raw_lat, lat_t, raw_in, raw_up, raw_low, raw_out,
    win, wmid, wupt, wup, wlow, wout_rows, wo, spread, g3x, g4x,
    latx, xs, first, a1, b1, b0, a3, act4, part, got, got_rows,
    wsem, lsend, lrecv, hsend, hrecv, psend, precv,
):
    frames, height, cw, c0, c1, c2, c3, colours = sizes
    ext = cw + 2
    wide = 2 * cw
    nc = wide + 2
    fc = frames * c0
    kinds = 2 * colours
    me = lax.axis_index("row")
    is_first, is_last = me == 0, me == devices - 1
    has_left, has_right = me > 0, me < devices - 1

    copies = {}

    def load(name, src, dst, k):
        copies[name] = pltpu.make_async_copy(src, dst, wsem.at[k])
        copies[name].start()

    load("lat", lat_hbm, latx.at[pl.ds(2, cw)] if packed else raw_lat, 0)
    load("in", win_hbm, raw_in, 1)
    load("out", wout_hbm, raw_out, 2)
    load("up", wup_hbm, raw_up, 3)
    load("low", wlow_hbm, raw_low, 4)
    for a in range(3):
        for b in range(3):
            load(("mid", a, b), wmid_hbm.at[a, b], wmid.at[:, b, :, pl.ds(a * c1, c1)], 5 + 3 * a + b)

    barrier = pltpu.get_barrier_semaphore()

    def greet(k, _):
        pl.semaphore_signal(barrier, inc=1, device_id={"row": lax.rem(me + k, devices)}, device_id_type=MESH)
        return _

    lax.fori_loop(1, devices, greet, 0)

    copies["lat"].wait()
    if not packed:
        chan, lane = iota((c0, LANES), 0), iota((c0, LANES), 1)
        total = None
        for t in range(frames):
            put = ((lane == t * c0 + chan) | (lane == fc + t * c0 + chan)).astype(bf16)
            field = raw_lat[t].astype(f32).reshape(height * cw, c0).astype(bf16)
            d = dot(field, put)
            total = d if total is None else total + d
        lat_t[...] = total
        for j in range(cw):
            latx[2 + j] = lat_t[pl.ds(j, height, stride=cw), :].astype(bf16)

    pl.semaphore_wait(barrier, devices - 1)

    def lat_copy(right):
        peer = me + 1 if right else me - 1
        src = latx.at[pl.ds(cw, 2)] if right else latx.at[pl.ds(2, 2)]
        dst = latx.at[pl.ds(0, 2)] if right else latx.at[pl.ds(cw + 2, 2)]
        return pltpu.make_async_remote_copy(
            src_ref=src, dst_ref=dst, send_sem=lsend.at[int(right)], recv_sem=lrecv.at[int(right)],
            device_id={"row": peer}, device_id_type=MESH,
        )

    @pl.when(has_right)
    def _():
        lat_copy(True).start()

    @pl.when(has_left)
    def _():
        lat_copy(False).start()

    @pl.when(is_first)
    def _():
        latx[0:2] = jnp.zeros((2, height, LANES), bf16)
        for t in range(frames):
            b1[t, 0] = jnp.zeros((height, c1), bf16)

    @pl.when(is_last)
    def _():
        latx[cw + 2 : cw + 4] = jnp.zeros((2, height, LANES), bf16)
        for t in range(frames):
            b1[t, ext - 1] = jnp.zeros((height, c1), bf16)

    copies["in"].wait()
    kx = 2 * LANES
    for e in range(3):
        for b in range(3):
            for s in range(frames):
                at = e * kx + b * fc + s * c0
                for t in range(frames):
                    a = s - t + 2
                    block = raw_in[a, b, e] if 0 <= a <= 2 else jnp.zeros((c0, c1), bf16)
                    win[at : at + c0, t * c1 : (t + 1) * c1] = block
        win[e * kx + 3 * fc : (e + 1) * kx, :] = jnp.zeros((kx - 3 * fc, frames * c1), bf16)

    hg1, hg2 = g1_ref[...] * 0.5, g2_ref[...] * 0.5
    g3x[0:1, 0:c2] = g3_ref[...] * 0.5
    g3x[0:1, c2 : 2 * c2] = g3_ref[...] * 0.5
    g4x[...] = jnp.zeros(g4x.shape, f32)
    g4x[0:1, 0:c3] = g4_ref[...] * 0.5

    copies["up"].wait()
    for row_odd in range(2):
        for in_row in range(2):
            mixed = []
            for e in range(3):
                if row_odd == 0:
                    taps = (0, 1) if in_row == 0 else (2,)
                else:
                    taps = (0,) if in_row == 0 else (1, 2)
                value = raw_up[taps[0], e].astype(f32)
                for b in taps[1:]:
                    value = value + raw_up[b, e].astype(f32)
                mixed.append(value)
            k0, k1, k2 = mixed
            for parity in range(2):
                pair = (k0 + k1, k2) if parity == 0 else (k0, k1 + k2)
                at = parity * 2 * c2 + row_odd * c2
                for in_col in range(2):
                    wupt[in_row, at : at + c2, in_col * c1 : (in_col + 1) * c1] = pair[in_col].astype(bf16)
    for in_row in range(2):
        for i in range(0, 4 * c2, LANES):
            for j in range(0, 2 * c1, LANES):
                wup[in_row, j : j + LANES, i : i + LANES] = wupt[in_row, i : i + LANES, j : j + LANES].T

    copies["low"].wait()
    for a in range(3):
        wlow[a] = jnp.zeros(wlow.shape[1:], bf16)
        for e in range(3):
            for b in range(3):
                block = raw_low[a, b, e]
                for q in range(2):
                    at = (4 * e + q + b) * c2
                    wlow[a, at : at + c2, q * LANES : q * LANES + c3] = block

    copies["out"].wait()
    tap_rows = wout_rows.shape[1]
    wout_rows[...] = jnp.zeros(wout_rows.shape, f32)
    for a in range(3):
        for b in range(3):
            for e in range(3):
                at = (3 * b + e) * colours
                wout_rows[a, at : at + colours, 0:c3] = raw_out[a, b, e].astype(f32)
    lane = iota((1, 6 * LANES), 1)
    tap_col = lane // (2 * LANES)
    group = (lane // LANES) % 2
    spot = lane % LANES
    kind = spot // nc
    row_kind, colour = kind // colours, kind % colours
    slot = jnp.where(group == 0, 1 + row_kind, 3 - 3 * row_kind)
    tap = iota((tap_rows, 6 * LANES), 0)
    for q in range(2):
        b = q - slot + 2
        wanted = jnp.where((b >= 0) & (b <= 2) & (kind < kinds), (3 * b + tap_col) * colours + colour, -1)
        select = (tap == wanted).astype(bf16)
        for a in range(3):
            wo[a, q * LANES : (q + 1) * LANES, :] = lax.dot_general(
                wout_rows[a].astype(bf16), select, (((0,), (0,)), ((), ())), preferred_element_type=f32
            ).astype(bf16)

    full = wide * devices
    spot = iota((LANES, full), 0)
    col = iota((LANES, full), 1) % wide
    for k in range(kinds):
        spread[:, k * full : (k + 1) * full] = (spot == k * nc + 1 + col).astype(bf16)

    @pl.when(has_left)
    def _():
        lat_copy(True).wait_recv()

    @pl.when(has_right)
    def _():
        lat_copy(False).wait_recv()

    h3 = iota((1, height, 1), 1)
    top3, bottom3 = h3 == 0, h3 == height - 1
    low_lanes = iota((1, 1, LANES), 2) < fc
    for j in range(0, cw + 4, 2):
        v = latx[j : j + 2].astype(f32)
        up = jnp.where(top3, 0.0, pltpu.roll(v, 1, 1))
        down = jnp.where(bottom3, 0.0, pltpu.roll(v, height - 1, 1))
        xs[j : j + 2, :, 0:LANES] = jnp.where(low_lanes, up, v).astype(bf16)
        xs[j : j + 2, :, LANES:kx] = jnp.where(low_lanes, down, 0.0).astype(bf16)

    lhs = jnp.concatenate([merge(xs[e : e + ext]) for e in range(3)], axis=-1)
    keep_left, keep_right = has_left.astype(f32), has_right.astype(f32)
    col_id = iota((ext * height, 1), 0)
    keep = jnp.where(col_id < height, keep_left, jnp.where(col_id >= (ext - 1) * height, keep_right, 1.0))
    for t in range(frames):
        total = dot(lhs, win[:, t * c1 : (t + 1) * c1])
        first[t] = total[height : (cw + 1) * height]
        act = rows_of(rms_act(total, hg1, c1) * keep, ext)
        up = jnp.where(top3, 0.0, pltpu.roll(act, 1, 1))
        down = jnp.where(bottom3, 0.0, pltpu.roll(act, height - 1, 1))
        a1[t, :, :, 0:c1] = up.astype(bf16)
        a1[t, :, :, c1 : 2 * c1] = act.astype(bf16)
        a1[t, :, :, 2 * c1 : 3 * c1] = down.astype(bf16)

    for a in range(3):
        for b in range(3):
            copies[("mid", a, b)].wait()

    def halo(t, right):
        peer = me + 1 if right else me - 1
        return pltpu.make_async_remote_copy(
            src_ref=b1.at[t, cw if right else 1], dst_ref=b1.at[t, 0 if right else ext - 1],
            send_sem=hsend.at[int(right), t], recv_sem=hrecv.at[int(right), t],
            device_id={"row": peer}, device_id_type=MESH,
        )

    sums = {t: [] for t in range(frames)}
    groups = [list(range(frames - 2)), [frames - 2], [frames - 1]]
    m = cw * height
    for group_of in groups:
        s0, n = group_of[0], len(group_of)
        least = max(0, 3 - (frames - s0))
        lhs = jnp.concatenate([merge(a1[s0 : s0 + n, e : e + cw]) for e in range(3)], axis=-1)
        d = dot(lhs, merge(wmid[:, :, :, least * c1 : 3 * c1]))
        for i, s in enumerate(group_of):
            for a in range(least, 3):
                t = s - a + 2
                sums[t].append(d[i * m : (i + 1) * m, (a - least) * c1 : (a - least + 1) * c1])
        for t in group_of:
            total = first[t]
            for v in sums[t]:
                total = total + v
            b1[t, 1 : cw + 1] = rows_of(rms_act(total, hg2, c1).astype(bf16), cw)

            @pl.when(has_right)
            def _(t=t):
                halo(t, True).start()

            @pl.when(has_left)
            def _(t=t):
                halo(t, False).start()

    low3 = iota((1, 2 * c2), 1) < c2
    pairs = cw + 1
    tall = iota((pairs * height, 1), 0)
    top = tall % height == 0
    bottom = tall % height == height - 1
    hg3, hg4 = g3x[...], g4x[...]

    def upsample(t):
        @pl.when(has_left)
        def _():
            halo(t, True).wait_recv()

        @pl.when(has_right)
        def _():
            halo(t, False).wait_recv()

        b0[t] = pltpu.roll(b1[t].astype(f32), 1, 1).astype(bf16)
        above = jnp.concatenate([merge(b0[t, e : e + pairs]) for e in range(2)], axis=-1)
        here = jnp.concatenate([merge(b1[t, e : e + pairs]) for e in range(2)], axis=-1)
        from_above, from_here = dot(above, wup[0]), dot(here, wup[1])
        for parity in range(2):
            span = slice(parity * 2 * c2, (parity + 1) * 2 * c2)
            field = jnp.where(top & ~low3, 0.0, from_above[:, span]) + jnp.where(top & low3, 0.0, from_here[:, span])
            act = pair_norm(field, hg3, low3)
            if parity == 0:
                act = act * jnp.where(tall < height, keep_left, 1.0)
            else:
                act = act * jnp.where(tall >= cw * height, keep_right, 1.0)
            act = rows_of(act, pairs)
            ahead = pltpu.roll(act, height - 1, 1)
            low = low3.reshape(1, 1, 2 * c2)
            a3[t, :, parity, :, 0 : 2 * c2] = jnp.where(top3 & low, 0.0, act).astype(bf16)
            a3[t, :, parity, :, 2 * c2 : 4 * c2] = jnp.where(bottom3 & ~low, 0.0, ahead).astype(bf16)

    lane_mod = iota((1, LANES), 1) % nc
    h2 = iota((height, 1), 0)
    even_kind = iota((1, LANES), 1) < colours * nc

    def message(t):
        def copy(k, act):
            peer = lax.rem(me + k, devices)
            return pltpu.make_async_remote_copy(
                src_ref=part.at[t, peer], dst_ref=got.at[t, me], send_sem=psend.at[t], recv_sem=precv.at[t],
                device_id={"row": peer}, device_id_type=MESH,
            )
        return copy

    def lower(t):
        total = None
        for a in range(3):
            s = t + a - 2
            if s < 0:
                continue
            field = a3[s].reshape(nc, height, 4 * c2)
            lhs = jnp.concatenate([merge(field[e : e + wide]) for e in range(3)], axis=-1)
            d = dot(lhs, wlow[a])
            total = d if total is None else total + d
        for q in range(2):
            span = slice(q * LANES, (q + 1) * LANES)
            act4[t, :, span] = rms_act(total[:, span], hg4, c3).astype(bf16)
        total = None
        for a in range(3):
            s = t + a - 2
            if s < 0:
                continue
            d = dot(act4[s], wo[a])
            total = d if total is None else total + d
        out = [None, None]
        for e in range(3):
            for c in range(wide):
                for g in range(2):
                    at = (2 * e + g) * LANES
                    v = jnp.where(lane_mod == c + 2 - e, total[c * height : (c + 1) * height, at : at + LANES], 0.0)
                    out[g] = v if out[g] is None else out[g] + v
        down = jnp.where(h2 == 0, 0.0, pltpu.roll(out[1], 1, 0))
        up = jnp.where(h2 == height - 1, 0.0, pltpu.roll(out[1], height - 1, 0))
        value = out[0] + jnp.where(even_kind, down, up)
        for d in range(devices):
            part[t, d] = value[d : d + 1]
        got[t, me] = part[t, me]

        def send(k, _):
            message(t)(k, None).start()
            return _

        lax.fori_loop(1, devices, send, 0)

    def all_sent(t, sem):
        return pltpu.make_async_copy(got.at[t, pl.ds(0, devices - 1)], got.at[t, pl.ds(0, devices - 1)], sem)

    source = iota((devices, 1), 0)
    cell = iota((devices, full), 1) // wide
    inside = (lane_mod >= 1) & (lane_mod <= wide)

    def finish(t):
        all_sent(t, precv.at[t]).wait()
        for d in range(devices):
            got_rows[d : d + 1] = got[t, d]
        g = got_rows[...]
        before = jnp.where((lane_mod == 0) & (source > 0), g, 0.0)
        after = jnp.where((lane_mod == nc - 1) & (source < devices - 1), g, 0.0)
        before = pltpu.roll(pltpu.roll(before, devices - 1, 0), wide, 1)
        after = pltpu.roll(pltpu.roll(after, 1, 0), LANES - wide, 1)
        g = jnp.where(inside, g, 0.0) + before + after
        high = g.astype(bf16)
        rest = g - high.astype(f32)
        middle = rest.astype(bf16)
        rest = rest - middle.astype(f32)
        d = dot(jnp.concatenate([high, middle, rest.astype(bf16)], axis=0), spread[...])
        d = d[0:devices] + d[devices : 2 * devices] + d[2 * devices : 3 * devices]
        for k in range(kinds):
            row = jnp.sum(jnp.where(cell == source, d[:, k * full : (k + 1) * full], 0.0), axis=0, keepdims=True)
            out_ref[t, k % colours, k // colours : k // colours + 1, :] = row

    for t in range(frames - 1):
        upsample(t)
    for t in range(frames - 1):
        lower(t)
    upsample(frames - 1)
    lower(frames - 1)
    for t in range(frames):
        finish(t)

    @pl.when(has_right)
    def _():
        lat_copy(True).wait_send()
        for t in range(frames):
            halo(t, True).wait_send()

    @pl.when(has_left)
    def _():
        lat_copy(False).wait_send()
        for t in range(frames):
            halo(t, False).wait_send()

    for t in range(frames):
        all_sent(t, psend.at[t]).wait()


def per_device(latent, w_in, gain_one, w_mid, gain_two, w_up, gain_three, w_low, gain_four, w_out):
    frames, height, cw, c0 = latent.shape
    devices = lax.axis_size("row")
    assert height == devices
    c1, c2, c3 = w_in.shape[-1], w_up.shape[-1], w_low.shape[-1]
    colours = w_out.shape[-1]
    ext, wide = cw + 2, 2 * cw
    full = wide * devices
    kinds = 2 * colours
    assert 2 * frames * c0 == LANES and kinds * (wide + 2) <= LANES
    packed = cw % 8 != 0
    if packed:
        lat = jnp.transpose(latent, (2, 1, 0, 3)).reshape(cw, height, frames * c0)
        lat = jnp.concatenate([lat, lat], axis=-1)
    else:
        lat = latent
    wup = jnp.transpose(w_up, (0, 1, 3, 2))
    wout = jnp.transpose(w_out, (0, 1, 2, 4, 3))
    tap_rows = -(-9 * colours // 16) * 16

    vmem = pl.BlockSpec(memory_space=pltpu.VMEM)
    hbm = pl.BlockSpec(memory_space=pl.ANY)
    dma = pltpu.SemaphoreType.DMA
    return pl.pallas_call(
        functools.partial(kernel, (frames, height, cw, c0, c1, c2, c3, colours), devices, packed),
        out_shape=jax.ShapeDtypeStruct((frames, colours, 2, full), f32),
        in_specs=[hbm] + [vmem] * 4 + [hbm] * 5,
        out_specs=vmem,
        scratch_shapes=[
            pltpu.VMEM(latent.shape, bf16),
            pltpu.VMEM((height * cw, LANES), f32),
            pltpu.VMEM(w_in.shape, bf16),
            pltpu.VMEM(wup.shape, bf16),
            pltpu.VMEM(w_low.shape, bf16),
            pltpu.VMEM(wout.shape, bf16),
            pltpu.VMEM((3 * 2 * LANES, frames * c1), bf16),
            pltpu.VMEM((3, 3, c1, 3 * c1), bf16),
            pltpu.VMEM((2, 4 * c2, 2 * c1), bf16),
            pltpu.VMEM((2, 2 * c1, 4 * c2), bf16),
            pltpu.VMEM((3, 12 * c2, 2 * LANES), bf16),
            pltpu.VMEM((3, tap_rows, LANES), f32),
            pltpu.VMEM((3, 2 * LANES, 6 * LANES), bf16),
            pltpu.VMEM((LANES, kinds * full), bf16),
            pltpu.VMEM((1, 2 * c2), f32),
            pltpu.VMEM((1, LANES), f32),
            pltpu.VMEM((cw + 4, height, LANES), bf16),
            pltpu.VMEM((cw + 4, height, 2 * LANES), bf16),
            pltpu.VMEM((frames, cw * height, c1), f32),
            pltpu.VMEM((frames, ext, height, 3 * c1), bf16),
            pltpu.VMEM((frames, ext, height, c1), bf16),
            pltpu.VMEM((frames, ext, height, c1), bf16),
            pltpu.VMEM((frames, cw + 1, 2, height, 4 * c2), bf16),
            pltpu.VMEM((frames, wide * height, 2 * LANES), bf16),
            pltpu.VMEM((frames, devices, 1, LANES), f32),
            pltpu.VMEM((frames, devices, 1, LANES), f32),
            pltpu.VMEM((devices, LANES), f32),
            dma((14,)), dma((2,)), dma((2,)), dma((2, frames)), dma((2, frames)), dma((frames,)), dma((frames,)),
        ],
        compiler_params=pltpu.CompilerParams(
            collective_id=0, has_side_effects=True, vmem_limit_bytes=60 * 1024 * 1024
        ),
    )(
        lat, gain_one.reshape(1, c1), gain_two.reshape(1, c1), gain_three.reshape(1, c2), gain_four.reshape(1, c3),
        w_in, w_mid, wup, w_low, wout,
    )


def solution(mesh):
    placed = (P("groups", None, "row", None), P(), P(), P(), P(), P(), P(), P(), P(), P())
    return jax.shard_map(
        per_device,
        mesh=mesh,
        in_specs=placed,
        out_specs=P("groups", None, "row", None),
        check_vma=False,
    )
```

```python
import functools

import jax
import jax.numpy as jnp
from jax import lax
from jax.experimental import pallas as pl
from jax.experimental.pallas import tpu as pltpu
from jax.sharding import PartitionSpec as P

eps = 1e-06
f32, bf16, i32 = jnp.float32, jnp.bfloat16, jnp.int32
MESH = pl.DeviceIdType.MESH
LANES = 128


def half_silu(h):
    return h * jnp.tanh(h) + h


def rms_act(field, half_gain, count):
    mean = jnp.sum(field * field, axis=-1, keepdims=True) * (1.0 / count)
    return half_silu(field * lax.rsqrt(mean + eps) * half_gain)


def pair_norm(field, half_gain, low):
    half = field.shape[-1] // 2
    square = field * field
    first = jnp.sum(jnp.where(low, square, 0.0), axis=-1, keepdims=True)
    second = jnp.sum(jnp.where(low, 0.0, square), axis=-1, keepdims=True)
    inv = 1.0 / half
    scale = jnp.where(low, lax.rsqrt(first * inv + eps), lax.rsqrt(second * inv + eps))
    return half_silu(field * scale * half_gain)


def dot(a, b):
    return jnp.dot(a, b, preferred_element_type=f32)


def iota(shape, axis):
    return lax.broadcasted_iota(i32, shape, axis)


def merge(value):
    return value.reshape(-1, value.shape[-1])


def rows_of(value, count):
    return value.reshape(count, value.shape[0] // count, value.shape[1])


def kernel(
    sizes, devices, packed,
    lat_hbm, g1_hbm, g2_hbm, g3_hbm, g4_hbm,
    win_hbm, wmid_hbm, wup_hbm, wlow_hbm, wout_hbm,
    out_ref,
    g1_ref, g2_ref, g3_ref, g4_ref, raw_lat, lat_t, raw_in, raw_up, raw_low, raw_out,
    win, wmid, wupt, wup, wlow, wout_rows, wo, spread, g3x, g4x,
    latx, xs, first, a1, b1, b0, a3, act4, part, got, got_rows,
    wsem, known, lsend, lrecv, hsend, hrecv, psend, precv,
):
    frames, height, cw, c0, c1, c2, c3, colours = sizes
    ext = cw + 2
    wide = 2 * cw
    nc = wide + 2
    fc = frames * c0
    kinds = 2 * colours
    me = lax.axis_index("row")
    is_first, is_last = me == 0, me == devices - 1
    has_left, has_right = me > 0, me < devices - 1

    copies = {}

    def load(name, src, dst, k):
        copies[name] = pltpu.make_async_copy(src, dst, wsem.at[k])
        copies[name].start()

    load("lat", lat_hbm, latx.at[pl.ds(2, cw)] if packed else raw_lat, 0)
    load("in", win_hbm, raw_in, 1)
    load("out", wout_hbm, raw_out, 2)
    gain_refs = [(g1_hbm, g1_ref), (g2_hbm, g2_ref), (g3_hbm, g3_ref), (g4_hbm, g4_ref)]
    for i, (src, dst) in enumerate(gain_refs):
        load(("gain", i), src, dst, 14 + i)
    load("up", wup_hbm, raw_up, 3)
    load("low", wlow_hbm, raw_low, 4)
    for a in range(3):
        for b in range(3):
            load(("mid", a, b), wmid_hbm.at[a, b], wmid.at[:, b, :, pl.ds(a * c1, c1)], 5 + 3 * a + b)

    barrier = pltpu.get_barrier_semaphore()

    for peer, there in ((me - 1, has_left), (me + 1, has_right)):
        @pl.when(there)
        def _(peer=peer):
            pl.semaphore_signal(barrier, inc=1, device_id={"row": peer}, device_id_type=MESH)

    def tell(level):
        step = 2**level
        for side, peer in ((0, me - step), (1, me + step)):
            @pl.when((peer >= 0) & (peer < devices))
            def _(side=side, peer=peer):
                pl.semaphore_signal(known.at[side, level], inc=1, device_id={"row": peer}, device_id_type=MESH)

    def hear(level):
        step = 2**level
        for side, peer in ((1, me - step), (0, me + step)):
            @pl.when((peer >= 0) & (peer < devices))
            def _(side=side):
                pl.semaphore_wait(known.at[side, level], 1)

    levels = known.shape[1]

    copies["lat"].wait()
    if not packed:
        chan, lane = iota((c0, LANES), 0), iota((c0, LANES), 1)
        total = None
        for t in range(frames):
            put = ((lane == t * c0 + chan) | (lane == fc + t * c0 + chan)).astype(bf16)
            field = raw_lat[t].astype(f32).reshape(height * cw, c0).astype(bf16)
            d = dot(field, put)
            total = d if total is None else total + d
        lat_t[...] = total
        for j in range(cw):
            latx[2 + j] = lat_t[pl.ds(j, height, stride=cw), :].astype(bf16)

    pl.semaphore_wait(barrier, has_left.astype(i32) + has_right.astype(i32))

    def lat_copy(right):
        peer = me + 1 if right else me - 1
        src = latx.at[pl.ds(cw, 2)] if right else latx.at[pl.ds(2, 2)]
        dst = latx.at[pl.ds(0, 2)] if right else latx.at[pl.ds(cw + 2, 2)]
        return pltpu.make_async_remote_copy(
            src_ref=src, dst_ref=dst, send_sem=lsend.at[int(right)], recv_sem=lrecv.at[int(right)],
            device_id={"row": peer}, device_id_type=MESH,
        )

    @pl.when(has_right)
    def _():
        lat_copy(True).start()

    @pl.when(has_left)
    def _():
        lat_copy(False).start()

    tell(0)

    @pl.when(is_first)
    def _():
        latx[0:2] = jnp.zeros((2, height, LANES), bf16)
        for t in range(frames):
            b1[t, 0] = jnp.zeros((height, c1), bf16)

    @pl.when(is_last)
    def _():
        latx[cw + 2 : cw + 4] = jnp.zeros((2, height, LANES), bf16)
        for t in range(frames):
            b1[t, ext - 1] = jnp.zeros((height, c1), bf16)

    copies["in"].wait()
    kx = 2 * LANES
    for e in range(3):
        for b in range(3):
            for s in range(frames):
                at = e * kx + b * fc + s * c0
                for t in range(frames):
                    a = s - t + 2
                    block = raw_in[a, b, e] if 0 <= a <= 2 else jnp.zeros((c0, c1), bf16)
                    win[at : at + c0, t * c1 : (t + 1) * c1] = block
        win[e * kx + 3 * fc : (e + 1) * kx, :] = jnp.zeros((kx - 3 * fc, frames * c1), bf16)

    for i in range(4):
        copies[("gain", i)].wait()

    def gain(ref):
        rows = ref[...] * 0.5
        return jnp.concatenate([rows[i : i + 1] for i in range(rows.shape[0])], axis=-1)

    hg1, hg2 = gain(g1_ref), gain(g2_ref)
    g3x[0:1, 0:c2] = g3_ref[...] * 0.5
    g3x[0:1, c2 : 2 * c2] = g3_ref[...] * 0.5
    g4x[...] = jnp.zeros(g4x.shape, f32)
    g4x[0:1, 0:c3] = g4_ref[...] * 0.5

    copies["up"].wait()
    for row_odd in range(2):
        for in_row in range(2):
            mixed = []
            for e in range(3):
                if row_odd == 0:
                    taps = (0, 1) if in_row == 0 else (2,)
                else:
                    taps = (0,) if in_row == 0 else (1, 2)
                value = raw_up[taps[0], e].astype(f32)
                for b in taps[1:]:
                    value = value + raw_up[b, e].astype(f32)
                mixed.append(value)
            k0, k1, k2 = mixed
            for parity in range(2):
                pair = (k0 + k1, k2) if parity == 0 else (k0, k1 + k2)
                at = parity * 2 * c2 + row_odd * c2
                for in_col in range(2):
                    wupt[in_row, at : at + c2, in_col * c1 : (in_col + 1) * c1] = pair[in_col].astype(bf16)
    for in_row in range(2):
        for i in range(0, 4 * c2, LANES):
            for j in range(0, 2 * c1, LANES):
                wup[in_row, j : j + LANES, i : i + LANES] = wupt[in_row, i : i + LANES, j : j + LANES].T

    copies["low"].wait()
    for a in range(3):
        wlow[a] = jnp.zeros(wlow.shape[1:], bf16)
        for e in range(3):
            for b in range(3):
                block = raw_low[a, b, e]
                for q in range(2):
                    at = (4 * e + q + b) * c2
                    wlow[a, at : at + c2, q * LANES : q * LANES + c3] = block

    copies["out"].wait()
    tap_rows = wout_rows.shape[1]
    wout_rows[...] = jnp.zeros(wout_rows.shape, f32)
    for a in range(3):
        for b in range(3):
            for e in range(3):
                at = (3 * b + e) * colours
                wout_rows[a, at : at + colours, 0:c3] = raw_out[a, b, e].astype(f32)
    lane = iota((1, 6 * LANES), 1)
    tap_col = lane // (2 * LANES)
    group = (lane // LANES) % 2
    spot = lane % LANES
    kind = spot // nc
    row_kind, colour = kind // colours, kind % colours
    slot = jnp.where(group == 0, 1 + row_kind, 3 - 3 * row_kind)
    tap = iota((tap_rows, 6 * LANES), 0)
    for q in range(2):
        b = q - slot + 2
        wanted = jnp.where((b >= 0) & (b <= 2) & (kind < kinds), (3 * b + tap_col) * colours + colour, -1)
        select = (tap == wanted).astype(bf16)
        for a in range(3):
            wo[a, q * LANES : (q + 1) * LANES, :] = lax.dot_general(
                wout_rows[a].astype(bf16), select, (((0,), (0,)), ((), ())), preferred_element_type=f32
            ).astype(bf16)

    full = wide * devices
    spot = iota((LANES, full), 0)
    col = iota((LANES, full), 1) % wide
    for k in range(kinds):
        spread[:, k * full : (k + 1) * full] = (spot == k * nc + 1 + col).astype(bf16)

    if 1 < levels:
        hear(0)
        tell(1)
    @pl.when(has_left)
    def _():
        lat_copy(True).wait_recv()

    @pl.when(has_right)
    def _():
        lat_copy(False).wait_recv()

    h3 = iota((1, height, 1), 1)
    top3, bottom3 = h3 == 0, h3 == height - 1
    low_lanes = iota((1, 1, LANES), 2) < fc
    for j in range(0, cw + 4, 2):
        v = latx[j : j + 2].astype(f32)
        up = jnp.where(top3, 0.0, pltpu.roll(v, 1, 1))
        down = jnp.where(bottom3, 0.0, pltpu.roll(v, height - 1, 1))
        xs[j : j + 2, :, 0:LANES] = jnp.where(low_lanes, up, v).astype(bf16)
        xs[j : j + 2, :, LANES:kx] = jnp.where(low_lanes, down, 0.0).astype(bf16)

    lhs = jnp.concatenate([merge(xs[e : e + ext]) for e in range(3)], axis=-1)
    keep_left, keep_right = has_left.astype(f32), has_right.astype(f32)
    col_id = iota((ext * height, 1), 0)
    keep = jnp.where(col_id < height, keep_left, jnp.where(col_id >= (ext - 1) * height, keep_right, 1.0))
    for t in range(frames):
        total = dot(lhs, win[:, t * c1 : (t + 1) * c1])
        first[t] = total[height : (cw + 1) * height]
        act = rows_of(rms_act(total, hg1, c1) * keep, ext)
        up = jnp.where(top3, 0.0, pltpu.roll(act, 1, 1))
        down = jnp.where(bottom3, 0.0, pltpu.roll(act, height - 1, 1))
        a1[t, :, :, 0:c1] = up.astype(bf16)
        a1[t, :, :, c1 : 2 * c1] = act.astype(bf16)
        a1[t, :, :, 2 * c1 : 3 * c1] = down.astype(bf16)

    if 2 < levels:
        hear(1)
        tell(2)
    for a in range(3):
        for b in range(3):
            copies[("mid", a, b)].wait()

    def halo(t, right):
        peer = me + 1 if right else me - 1
        return pltpu.make_async_remote_copy(
            src_ref=b1.at[t, cw if right else 1], dst_ref=b1.at[t, 0 if right else ext - 1],
            send_sem=hsend.at[int(right), t], recv_sem=hrecv.at[int(right), t],
            device_id={"row": peer}, device_id_type=MESH,
        )

    sums = {t: [] for t in range(frames)}
    groups = [list(range(frames - 2)), [frames - 2], [frames - 1]]
    m = cw * height
    for group_of in groups:
        s0, n = group_of[0], len(group_of)
        least = max(0, 3 - (frames - s0))
        lhs = jnp.concatenate([merge(a1[s0 : s0 + n, e : e + cw]) for e in range(3)], axis=-1)
        rhs = merge(wmid[:, :, :, least * c1 : 3 * c1])
        paired = rhs.shape[1] // 512 * 512
        cut = rhs.shape[0] // 512 * 256 + (256 if rhs.shape[0] % 512 else 0)
        d = dot(lhs[:, :cut], rhs[:cut, paired:]) + dot(lhs[:, cut:], rhs[cut:, paired:])
        if paired:
            d = jnp.concatenate([dot(lhs, rhs[:, :paired]), d], axis=-1)
        for i, s in enumerate(group_of):
            for a in range(least, 3):
                t = s - a + 2
                sums[t].append(d[i * m : (i + 1) * m, (a - least) * c1 : (a - least + 1) * c1])
        for t in group_of:
            total = first[t]
            for v in sums[t]:
                total = total + v
            b1[t, 1 : cw + 1] = rows_of(rms_act(total, hg2, c1).astype(bf16), cw)

            @pl.when(has_right)
            def _(t=t):
                halo(t, True).start()

            @pl.when(has_left)
            def _(t=t):
                halo(t, False).start()

    low3 = iota((1, 2 * c2), 1) < c2
    pairs = cw + 1
    tall = iota((pairs * height, 1), 0)
    top = tall % height == 0
    bottom = tall % height == height - 1
    hg3, hg4 = g3x[...], g4x[...]

    def upsample(t):
        @pl.when(has_left)
        def _():
            halo(t, True).wait_recv()

        @pl.when(has_right)
        def _():
            halo(t, False).wait_recv()

        b0[t] = pltpu.roll(b1[t].astype(f32), 1, 1).astype(bf16)
        above = jnp.concatenate([merge(b0[t, e : e + pairs]) for e in range(2)], axis=-1)
        here = jnp.concatenate([merge(b1[t, e : e + pairs]) for e in range(2)], axis=-1)
        from_above, from_here = dot(above, wup[0]), dot(here, wup[1])
        for parity in range(2):
            span = slice(parity * 2 * c2, (parity + 1) * 2 * c2)
            field = jnp.where(top & ~low3, 0.0, from_above[:, span]) + jnp.where(top & low3, 0.0, from_here[:, span])
            act = pair_norm(field, hg3, low3)
            if parity == 0:
                act = act * jnp.where(tall < height, keep_left, 1.0)
            else:
                act = act * jnp.where(tall >= cw * height, keep_right, 1.0)
            act = rows_of(act, pairs)
            ahead = pltpu.roll(act, height - 1, 1)
            low = low3.reshape(1, 1, 2 * c2)
            a3[t, :, parity, :, 0 : 2 * c2] = jnp.where(top3 & low, 0.0, act).astype(bf16)
            a3[t, :, parity, :, 2 * c2 : 4 * c2] = jnp.where(bottom3 & ~low, 0.0, ahead).astype(bf16)

    lane_mod = iota((1, LANES), 1) % nc
    h2 = iota((height, 1), 0)
    even_kind = iota((1, LANES), 1) < colours * nc

    for level in range(3, levels):
        hear(level - 1)
        tell(level)
    hear(levels - 1)

    def message(t):
        def copy(k, act):
            peer = lax.rem(me + k, devices)
            return pltpu.make_async_remote_copy(
                src_ref=part.at[t, peer], dst_ref=got.at[t, me], send_sem=psend.at[t], recv_sem=precv.at[t],
                device_id={"row": peer}, device_id_type=MESH,
            )
        return copy

    def lower(t):
        half = wide // 2 * height
        for i in range(2):
            total = None
            for a in range(3):
                s = t + a - 2
                if s < 0:
                    continue
                field = a3[s].reshape(nc, height, 4 * c2)
                c = i * wide // 2
                lhs = jnp.concatenate([merge(field[c + e : c + e + wide // 2]) for e in range(3)], axis=-1)
                d = dot(lhs, wlow[a])
                total = d if total is None else total + d
            for q in range(2):
                span = slice(q * LANES, (q + 1) * LANES)
                act4[t, i * half : (i + 1) * half, span] = rms_act(total[:, span], hg4, c3).astype(bf16)
        main, rest = None, [None, None]
        for a in range(3):
            s = t + a - 2
            if s < 0:
                continue
            d = dot(act4[s], wo[a, :, : 4 * LANES])
            main = d if main is None else main + d
            for i in range(2):
                d = dot(act4[s, i * half : (i + 1) * half], wo[a, :, 4 * LANES :])
                rest[i] = d if rest[i] is None else rest[i] + d
        total = jnp.concatenate([main, jnp.concatenate(rest, axis=0)], axis=-1)
        out = [None, None]
        for e in range(3):
            for c in range(wide):
                for g in range(2):
                    at = (2 * e + g) * LANES
                    v = jnp.where(lane_mod == c + 2 - e, total[c * height : (c + 1) * height, at : at + LANES], 0.0)
                    out[g] = v if out[g] is None else out[g] + v
        down = jnp.where(h2 == 0, 0.0, pltpu.roll(out[1], 1, 0))
        up = jnp.where(h2 == height - 1, 0.0, pltpu.roll(out[1], height - 1, 0))
        value = out[0] + jnp.where(even_kind, down, up)
        for d in range(devices):
            part[t, d] = value[d : d + 1]
        got[t, me] = part[t, me]

        def send(k, _):
            message(t)(k, None).start()
            return _

        lax.fori_loop(1, devices, send, 0)

    def all_sent(t, sem):
        return pltpu.make_async_copy(got.at[t, pl.ds(0, devices - 1)], got.at[t, pl.ds(0, devices - 1)], sem)

    source = iota((devices, 1), 0)
    cell = iota((devices, full), 1) // wide
    inside = (lane_mod >= 1) & (lane_mod <= wide)

    def finish(t):
        all_sent(t, precv.at[t]).wait()
        for d in range(devices):
            got_rows[d : d + 1] = got[t, d]
        g = got_rows[...]
        before = jnp.where((lane_mod == 0) & (source > 0), g, 0.0)
        after = jnp.where((lane_mod == nc - 1) & (source < devices - 1), g, 0.0)
        before = pltpu.roll(pltpu.roll(before, devices - 1, 0), wide, 1)
        after = pltpu.roll(pltpu.roll(after, 1, 0), LANES - wide, 1)
        g = jnp.where(inside, g, 0.0) + before + after
        high = g.astype(bf16)
        rest = g - high.astype(f32)
        middle = rest.astype(bf16)
        rest = rest - middle.astype(f32)
        d = dot(jnp.concatenate([high, middle, rest.astype(bf16)], axis=0), spread[...])
        d = d[0:devices] + d[devices : 2 * devices] + d[2 * devices : 3 * devices]
        for k in range(kinds):
            row = jnp.sum(jnp.where(cell == source, d[:, k * full : (k + 1) * full], 0.0), axis=0, keepdims=True)
            out_ref[t, k % colours, k // colours : k // colours + 1, :] = row

    for t in range(frames - 1):
        upsample(t)
    for t in range(frames - 1):
        lower(t)
    upsample(frames - 1)
    lower(frames - 1)
    for t in range(frames):
        if t == frames - 1:
            pass
        finish(t)

    @pl.when(has_right)
    def _():
        lat_copy(True).wait_send()
        for t in range(frames):
            halo(t, True).wait_send()

    @pl.when(has_left)
    def _():
        lat_copy(False).wait_send()
        for t in range(frames):
            halo(t, False).wait_send()

    for t in range(frames):
        all_sent(t, psend.at[t]).wait()


def per_device(latent, w_in, gain_one, w_mid, gain_two, w_up, gain_three, w_low, gain_four, w_out):
    frames, height, cw, c0 = latent.shape
    devices = lax.axis_size("row")
    assert height == devices
    c1, c2, c3 = w_in.shape[-1], w_up.shape[-1], w_low.shape[-1]
    colours = w_out.shape[-1]
    ext, wide = cw + 2, 2 * cw
    full = wide * devices
    kinds = 2 * colours
    levels = max(1, (devices - 1).bit_length())
    assert 2 * frames * c0 == LANES and kinds * (wide + 2) <= LANES
    packed = cw % 8 != 0
    if packed:
        lat = jnp.transpose(latent, (2, 1, 0, 3)).reshape(cw, height, frames * c0)
        lat = jnp.concatenate([lat, lat], axis=-1)
    else:
        lat = latent
    wup = jnp.transpose(w_up, (0, 1, 3, 2))
    wout = jnp.transpose(w_out, (0, 1, 2, 4, 3))
    tap_rows = -(-9 * colours // 16) * 16

    vmem = pl.BlockSpec(memory_space=pltpu.VMEM)
    hbm = pl.BlockSpec(memory_space=pltpu.HBM)
    dma = pltpu.SemaphoreType.DMA
    return pl.pallas_call(
        functools.partial(kernel, (frames, height, cw, c0, c1, c2, c3, colours), devices, packed),
        out_shape=jax.ShapeDtypeStruct((frames, colours, 2, full), f32),
        in_specs=[hbm] * 10,
        out_specs=vmem,
        scratch_shapes=[
            pltpu.VMEM((c1 // LANES, LANES), f32),
            pltpu.VMEM((c1 // LANES, LANES), f32),
            pltpu.VMEM((1, c2), f32),
            pltpu.VMEM((1, c3), f32),
            pltpu.VMEM(latent.shape, bf16),
            pltpu.VMEM((height * cw, LANES), f32),
            pltpu.VMEM(w_in.shape, bf16),
            pltpu.VMEM(wup.shape, bf16),
            pltpu.VMEM(w_low.shape, bf16),
            pltpu.VMEM(wout.shape, bf16),
            pltpu.VMEM((3 * 2 * LANES, frames * c1), bf16),
            pltpu.VMEM((3, 3, c1, 3 * c1), bf16),
            pltpu.VMEM((2, 4 * c2, 2 * c1), bf16),
            pltpu.VMEM((2, 2 * c1, 4 * c2), bf16),
            pltpu.VMEM((3, 12 * c2, 2 * LANES), bf16),
            pltpu.VMEM((3, tap_rows, LANES), f32),
            pltpu.VMEM((3, 2 * LANES, 6 * LANES), bf16),
            pltpu.VMEM((LANES, kinds * full), bf16),
            pltpu.VMEM((1, 2 * c2), f32),
            pltpu.VMEM((1, LANES), f32),
            pltpu.VMEM((cw + 4, height, LANES), bf16),
            pltpu.VMEM((cw + 4, height, 2 * LANES), bf16),
            pltpu.VMEM((frames, cw * height, c1), f32),
            pltpu.VMEM((frames, ext, height, 3 * c1), bf16),
            pltpu.VMEM((frames, ext, height, c1), bf16),
            pltpu.VMEM((frames, ext, height, c1), bf16),
            pltpu.VMEM((frames, cw + 1, 2, height, 4 * c2), bf16),
            pltpu.VMEM((frames, wide * height, 2 * LANES), bf16),
            pltpu.VMEM((frames, devices, 1, LANES), f32),
            pltpu.VMEM((frames, devices, 1, LANES), f32),
            pltpu.VMEM((devices, LANES), f32),
            dma((18,)), pltpu.SemaphoreType.REGULAR((2, levels)), dma((2,)), dma((2,)), dma((2, frames)), dma((2, frames)), dma((frames,)), dma((frames,)),
        ],
        compiler_params=pltpu.CompilerParams(
            collective_id=0, has_side_effects=True, vmem_limit_bytes=57 * 1024 * 1024
        ),
    )(
        lat, gain_one.reshape(-1, LANES), gain_two.reshape(-1, LANES), gain_three.reshape(1, c2), gain_four.reshape(1, c3),
        w_in, w_mid, wup, w_low, wout,
    )


def solution(mesh):
    placed = (P("groups", None, "row", None), P(), P(), P(), P(), P(), P(), P(), P(), P())
    return jax.shard_map(
        per_device,
        mesh=mesh,
        in_specs=placed,
        out_specs=P("groups", None, "row", None),
        check_vma=False,
    )
```

```python
import functools

import jax
import jax.numpy as jnp
from jax import lax
from jax.experimental import pallas as pl
from jax.experimental.pallas import tpu as pltpu
from jax.sharding import PartitionSpec as P

eps = 1e-06
f32, bf16, i32 = jnp.float32, jnp.bfloat16, jnp.int32
MESH = pl.DeviceIdType.MESH
LANES = 128


def half_silu(h):
    return h * jnp.tanh(h) + h


def rms_act(field, half_gain, count):
    mean = jnp.sum(field * field, axis=-1, keepdims=True) * (1.0 / count)
    return half_silu(field * lax.rsqrt(mean + eps) * half_gain)


def pair_norm(field, half_gain, low):
    half = field.shape[-1] // 2
    square = field * field
    first = jnp.sum(jnp.where(low, square, 0.0), axis=-1, keepdims=True)
    second = jnp.sum(jnp.where(low, 0.0, square), axis=-1, keepdims=True)
    inv = 1.0 / half
    scale = jnp.where(low, lax.rsqrt(first * inv + eps), lax.rsqrt(second * inv + eps))
    return half_silu(field * scale * half_gain)


def dot(a, b):
    return jnp.dot(a, b, preferred_element_type=f32)


def iota(shape, axis):
    return lax.broadcasted_iota(i32, shape, axis)


def merge(value):
    return value.reshape(-1, value.shape[-1])


def rows_of(value, count):
    return value.reshape(count, value.shape[0] // count, value.shape[1])


def kernel(
    sizes, devices, packed,
    lat_hbm, g1_hbm, g2_hbm, g3_hbm, g4_hbm,
    win_hbm, wmid_hbm, wup_hbm, wlow_hbm, wout_hbm,
    out_ref,
    g1_ref, g2_ref, g3_ref, g4_ref, raw_lat, lat_t, raw_in, raw_up, raw_low, raw_out,
    win, wmid, wupt, wup, wlow, wout_rows, wo, spread, g3x, g4x,
    latx, xs, first, a1, b1, b0, a3, act4, part, got, got_rows,
    wsem, known, lsend, lrecv, hsend, hrecv, psend, precv,
):
    frames, height, cw, c0, c1, c2, c3, colours = sizes
    ext = cw + 2
    wide = 2 * cw
    nc = wide + 2
    fc = frames * c0
    kinds = 2 * colours
    me = lax.axis_index("row")
    is_first, is_last = me == 0, me == devices - 1
    has_left, has_right = me > 0, me < devices - 1

    copies = {}

    def load(name, src, dst, k):
        copies[name] = pltpu.make_async_copy(src, dst, wsem.at[k])
        copies[name].start()

    load("lat", lat_hbm, latx.at[pl.ds(2, cw)] if packed else raw_lat, 0)
    load("in", win_hbm, raw_in, 1)
    gain_refs = [(g1_hbm, g1_ref), (g2_hbm, g2_ref), (g3_hbm, g3_ref), (g4_hbm, g4_ref)]
    for i, (src, dst) in enumerate(gain_refs):
        load(("gain", i), src, dst, 14 + i)
    load("out", wout_hbm, raw_out, 2)
    load("low", wlow_hbm, raw_low, 4)
    for a in range(3):
        for b in range(3):
            load(("mid", a, b), wmid_hbm.at[a, b], wmid.at[:, b, :, pl.ds(a * c1, c1)], 5 + 3 * a + b)
    load("up", wup_hbm, raw_up, 3)

    barrier = pltpu.get_barrier_semaphore()

    for peer, there in ((me - 1, has_left), (me + 1, has_right)):
        @pl.when(there)
        def _(peer=peer):
            pl.semaphore_signal(barrier, inc=1, device_id={"row": peer}, device_id_type=MESH)

    def tell(level):
        step = 2**level
        for side, peer in ((0, me - step), (1, me + step)):
            @pl.when((peer >= 0) & (peer < devices))
            def _(side=side, peer=peer):
                pl.semaphore_signal(known.at[side, level], inc=1, device_id={"row": peer}, device_id_type=MESH)

    def hear(level):
        step = 2**level
        for side, peer in ((1, me - step), (0, me + step)):
            @pl.when((peer >= 0) & (peer < devices))
            def _(side=side):
                pl.semaphore_wait(known.at[side, level], 1)

    levels = known.shape[1]

    copies["lat"].wait()
    if not packed:
        chan, lane = iota((c0, LANES), 0), iota((c0, LANES), 1)
        total = None
        for t in range(frames):
            put = ((lane == t * c0 + chan) | (lane == fc + t * c0 + chan)).astype(bf16)
            field = raw_lat[t].astype(f32).reshape(height * cw, c0).astype(bf16)
            d = dot(field, put)
            total = d if total is None else total + d
        lat_t[...] = total
        for j in range(cw):
            latx[2 + j] = lat_t[pl.ds(j, height, stride=cw), :].astype(bf16)

    pl.semaphore_wait(barrier, has_left.astype(i32) + has_right.astype(i32))

    def lat_copy(right):
        peer = me + 1 if right else me - 1
        src = latx.at[pl.ds(cw, 2)] if right else latx.at[pl.ds(2, 2)]
        dst = latx.at[pl.ds(0, 2)] if right else latx.at[pl.ds(cw + 2, 2)]
        return pltpu.make_async_remote_copy(
            src_ref=src, dst_ref=dst, send_sem=lsend.at[int(right)], recv_sem=lrecv.at[int(right)],
            device_id={"row": peer}, device_id_type=MESH,
        )

    @pl.when(has_right)
    def _():
        lat_copy(True).start()

    @pl.when(has_left)
    def _():
        lat_copy(False).start()

    tell(0)

    @pl.when(is_first)
    def _():
        latx[0:2] = jnp.zeros((2, height, LANES), bf16)
        for t in range(frames):
            b1[t, 0] = jnp.zeros((height, c1), bf16)

    @pl.when(is_last)
    def _():
        latx[cw + 2 : cw + 4] = jnp.zeros((2, height, LANES), bf16)
        for t in range(frames):
            b1[t, ext - 1] = jnp.zeros((height, c1), bf16)

    copies["in"].wait()
    kx = 2 * LANES
    for e in range(3):
        for b in range(3):
            for s in range(frames):
                at = e * kx + b * fc + s * c0
                for t in range(frames):
                    a = s - t + 2
                    block = raw_in[a, b, e] if 0 <= a <= 2 else jnp.zeros((c0, c1), bf16)
                    win[at : at + c0, t * c1 : (t + 1) * c1] = block
        win[e * kx + 3 * fc : (e + 1) * kx, :] = jnp.zeros((kx - 3 * fc, frames * c1), bf16)

    for i in range(4):
        copies[("gain", i)].wait()

    def gain(ref):
        rows = ref[...] * 0.5
        return jnp.concatenate([rows[i : i + 1] for i in range(rows.shape[0])], axis=-1)

    hg1, hg2 = gain(g1_ref), gain(g2_ref)
    g3x[0:1, 0:c2] = g3_ref[...] * 0.5
    g3x[0:1, c2 : 2 * c2] = g3_ref[...] * 0.5
    g4x[...] = jnp.zeros(g4x.shape, f32)
    g4x[0:1, 0:c3] = g4_ref[...] * 0.5

    copies["low"].wait()
    for a in range(3):
        wlow[a] = jnp.zeros(wlow.shape[1:], bf16)
        for e in range(3):
            for b in range(3):
                block = raw_low[a, b, e]
                for q in range(2):
                    at = (4 * e + q + b) * c2
                    wlow[a, at : at + c2, q * LANES : q * LANES + c3] = block

    copies["out"].wait()
    tap_rows = wout_rows.shape[1]
    wout_rows[...] = jnp.zeros(wout_rows.shape, f32)
    for a in range(3):
        for b in range(3):
            for e in range(3):
                at = (3 * b + e) * colours
                wout_rows[a, at : at + colours, 0:c3] = raw_out[a, b, e].astype(f32)
    lane = iota((1, 6 * LANES), 1)
    tap_col = lane // (2 * LANES)
    group = (lane // LANES) % 2
    spot = lane % LANES
    kind = spot // nc
    row_kind, colour = kind // colours, kind % colours
    slot = jnp.where(group == 0, 1 + row_kind, 3 - 3 * row_kind)
    tap = iota((tap_rows, 6 * LANES), 0)
    for q in range(2):
        b = q - slot + 2
        wanted = jnp.where((b >= 0) & (b <= 2) & (kind < kinds), (3 * b + tap_col) * colours + colour, -1)
        select = (tap == wanted).astype(bf16)
        for a in range(3):
            wo[a, q * LANES : (q + 1) * LANES, :] = lax.dot_general(
                wout_rows[a].astype(bf16), select, (((0,), (0,)), ((), ())), preferred_element_type=f32
            ).astype(bf16)

    full = wide * devices
    spot = iota((LANES, full), 0)
    col = iota((LANES, full), 1) % wide
    for k in range(kinds):
        spread[:, k * full : (k + 1) * full] = (spot == k * nc + 1 + col).astype(bf16)

    if 1 < levels:
        hear(0)
        tell(1)

    h3 = iota((1, height, 1), 1)
    top3, bottom3 = h3 == 0, h3 == height - 1
    low_lanes = iota((1, 1, LANES), 2) < fc
    keep_left, keep_right = has_left.astype(f32), has_right.astype(f32)

    def shift_rows(value):
        up = jnp.where(top3, 0.0, pltpu.roll(value, 1, 1))
        down = jnp.where(bottom3, 0.0, pltpu.roll(value, height - 1, 1))
        return up, down

    def stack_rows(j, n):
        v = latx[j : j + n].astype(f32)
        up, down = shift_rows(v)
        xs[j : j + n, :, 0:LANES] = jnp.where(low_lanes, up, v).astype(bf16)
        xs[j : j + n, :, LANES:kx] = jnp.where(low_lanes, down, 0.0).astype(bf16)

    def first_conv(spans, keep):
        lhs = jnp.concatenate(
            [merge(jnp.concatenate([xs[j + e : j + e + n] for j, n in spans], axis=0)) for e in range(3)], axis=-1
        )
        for t in range(frames):
            total = dot(lhs, win[:, t * c1 : (t + 1) * c1])
            act = rms_act(total, hg1, c1)
            if keep is not None:
                act = act * keep
            act = rows_of(act, act.shape[0] // height)
            up, down = shift_rows(act)
            at = 0
            for j, n in spans:
                for c in range(max(j, 1), min(j + n, cw + 1)):
                    first[t, (c - 1) * height : c * height] = total[(at + c - j) * height : (at + c - j + 1) * height]
                for k, value in enumerate((up, act, down)):
                    a1[t, j : j + n, :, k * c1 : (k + 1) * c1] = value[at : at + n].astype(bf16)
                at += n

    stack_rows(2, cw)
    if cw > 2:
        first_conv([(2, cw - 2)], None)

    @pl.when(has_left)
    def _():
        lat_copy(True).wait_recv()

    @pl.when(has_right)
    def _():
        lat_copy(False).wait_recv()

    stack_rows(0, 2)
    stack_rows(cw + 2, 2)
    place = iota((4 * height, 1), 0)
    keep = jnp.where(place < height, keep_left, jnp.where(place >= 3 * height, keep_right, 1.0))
    first_conv([(0, 2), (ext - 2, 2)], keep)

    if 2 < levels:
        hear(1)
        tell(2)

    for a in range(3):
        for b in range(3):
            copies[("mid", a, b)].wait()

    def halo(t, right):
        peer = me + 1 if right else me - 1
        return pltpu.make_async_remote_copy(
            src_ref=b1.at[t, cw if right else 1], dst_ref=b1.at[t, 0 if right else ext - 1],
            send_sem=hsend.at[int(right), t], recv_sem=hrecv.at[int(right), t],
            device_id={"row": peer}, device_id_type=MESH,
        )

    def mix_up():
        for row_odd in range(2):
            for in_row in range(2):
                mixed = []
                for e in range(3):
                    if row_odd == 0:
                        taps = (0, 1) if in_row == 0 else (2,)
                    else:
                        taps = (0,) if in_row == 0 else (1, 2)
                    value = raw_up[taps[0], e].astype(f32)
                    for b in taps[1:]:
                        value = value + raw_up[b, e].astype(f32)
                    mixed.append(value)
                k0, k1, k2 = mixed
                for parity in range(2):
                    pair = (k0 + k1, k2) if parity == 0 else (k0, k1 + k2)
                    at = parity * 2 * c2 + row_odd * c2
                    for in_col in range(2):
                        wupt[in_row, at : at + c2, in_col * c1 : (in_col + 1) * c1] = pair[in_col].astype(bf16)
        for in_row in range(2):
            for i in range(0, 4 * c2, LANES):
                for j in range(0, 2 * c1, LANES):
                    wup[in_row, j : j + LANES, i : i + LANES] = wupt[in_row, i : i + LANES, j : j + LANES].T

    copies["up"].wait()
    sums = {t: [] for t in range(frames)}
    m = cw * height
    tasks = [(0, 1, 2), (1, 2, 2), (0, 0, 0), (1, 0, 1)]
    tasks = [(s, low, high) for s, low, high in tasks if s - high + 2 < frames]
    tasks += [(s, max(0, 3 - frames + s), 2) for s in range(2, frames)]
    assert frames >= 3
    left = {t: min(3, t + 1) for t in range(frames)}
    sent_count = 0
    for s, least, most in tasks:
        least = max(least, 3 - frames + s)
        lhs = jnp.concatenate([merge(a1[s, e : e + cw]) for e in range(3)], axis=-1)
        rhs = merge(wmid[:, :, :, least * c1 : (most + 1) * c1])
        paired = rhs.shape[1] // 512 * 512
        cut = rhs.shape[0] // 512 * 256 + (256 if rhs.shape[0] % 512 else 0)
        d = dot(lhs[:, :cut], rhs[:cut, paired:]) + dot(lhs[:, cut:], rhs[cut:, paired:])
        if paired:
            d = jnp.concatenate([dot(lhs, rhs[:, :paired]), d], axis=-1)
        done = []
        for a in range(least, most + 1):
            t = s - a + 2
            sums[t].append(d[:, (a - least) * c1 : (a - least + 1) * c1])
            left[t] -= 1
            if left[t] == 0:
                done.append(t)
        for t in done:
            total = first[t]
            for v in sums[t]:
                total = total + v
            b1[t, 1 : cw + 1] = rows_of(rms_act(total, hg2, c1).astype(bf16), cw)
            sent_count += 1

        if done and sent_count > 1:
            times = list(range(2)) if sent_count == 2 else done

            @pl.when(has_right)
            def _(times=times):
                for t in times:
                    halo(t, True).start()

            @pl.when(has_left)
            def _(times=times):
                for t in times:
                    halo(t, False).start()

            if levels > 3 and sent_count == 2:
                hear(2)
                tell(3)
            if sent_count == 2:
                mix_up()
            if sent_count == frames:
                for level in range(4, levels):
                    hear(level - 1)
                    tell(level)

    low3 = iota((1, 2 * c2), 1) < c2
    pairs = cw + 1
    tall = iota((pairs * height, 1), 0)
    top = tall % height == 0
    bottom = tall % height == height - 1
    hg3, hg4 = g3x[...], g4x[...]

    def arrive(times):
        @pl.when(has_left)
        def _():
            for t in times:
                halo(t, True).wait_recv()

        @pl.when(has_right)
        def _():
            for t in times:
                halo(t, False).wait_recv()

    def upsample(t):
        b0[t] = pltpu.roll(b1[t].astype(f32), 1, 1).astype(bf16)
        above = jnp.concatenate([merge(b0[t, e : e + pairs]) for e in range(2)], axis=-1)
        here = jnp.concatenate([merge(b1[t, e : e + pairs]) for e in range(2)], axis=-1)
        from_above, from_here = dot(above, wup[0]), dot(here, wup[1])
        for parity in range(2):
            span = slice(parity * 2 * c2, (parity + 1) * 2 * c2)
            field = jnp.where(top & ~low3, 0.0, from_above[:, span]) + jnp.where(top & low3, 0.0, from_here[:, span])
            act = pair_norm(field, hg3, low3)
            if parity == 0:
                act = act * jnp.where(tall < height, keep_left, 1.0)
            else:
                act = act * jnp.where(tall >= cw * height, keep_right, 1.0)
            act = rows_of(act, pairs)
            ahead = pltpu.roll(act, height - 1, 1)
            low = low3.reshape(1, 1, 2 * c2)
            a3[t, :, parity, :, 0 : 2 * c2] = jnp.where(top3 & low, 0.0, act).astype(bf16)
            a3[t, :, parity, :, 2 * c2 : 4 * c2] = jnp.where(bottom3 & ~low, 0.0, ahead).astype(bf16)

    lane_mod = iota((1, LANES), 1) % nc
    h2 = iota((height, 1), 0)
    even_kind = iota((1, LANES), 1) < colours * nc

    def message(t):
        def copy(k, act):
            peer = lax.rem(me + k, devices)
            return pltpu.make_async_remote_copy(
                src_ref=part.at[t, peer], dst_ref=got.at[t, me], send_sem=psend.at[t], recv_sem=precv.at[t],
                device_id={"row": peer}, device_id_type=MESH,
            )
        return copy

    def lower(t):
        half = wide // 2 * height
        for i in range(2):
            total = None
            for a in range(3):
                s = t + a - 2
                if s < 0:
                    continue
                field = a3[s].reshape(nc, height, 4 * c2)
                c = i * wide // 2
                lhs = jnp.concatenate([merge(field[c + e : c + e + wide // 2]) for e in range(3)], axis=-1)
                d = dot(lhs, wlow[a])
                total = d if total is None else total + d
            for q in range(2):
                span = slice(q * LANES, (q + 1) * LANES)
                act4[t, i * half : (i + 1) * half, span] = rms_act(total[:, span], hg4, c3).astype(bf16)
        main, rest = None, [None, None]
        for a in range(3):
            s = t + a - 2
            if s < 0:
                continue
            d = dot(act4[s], wo[a, :, : 4 * LANES])
            main = d if main is None else main + d
            for i in range(2):
                d = dot(act4[s, i * half : (i + 1) * half], wo[a, :, 4 * LANES :])
                rest[i] = d if rest[i] is None else rest[i] + d
        total = jnp.concatenate([main, jnp.concatenate(rest, axis=0)], axis=-1)
        out = [None, None]
        for e in range(3):
            for c in range(wide):
                for g in range(2):
                    at = (2 * e + g) * LANES
                    v = jnp.where(lane_mod == c + 2 - e, total[c * height : (c + 1) * height, at : at + LANES], 0.0)
                    out[g] = v if out[g] is None else out[g] + v
        down = jnp.where(h2 == 0, 0.0, pltpu.roll(out[1], 1, 0))
        up = jnp.where(h2 == height - 1, 0.0, pltpu.roll(out[1], height - 1, 0))
        value = out[0] + jnp.where(even_kind, down, up)
        for d in range(devices):
            part[t, d] = value[d : d + 1]
        got[t, me] = part[t, me]

    def send_all(times):
        def send(k, _):
            for t in times:
                message(t)(k, None).start()
            return _

        lax.fori_loop(1, devices, send, 0)

    def all_sent(t, sem):
        return pltpu.make_async_copy(got.at[t, pl.ds(0, devices - 1)], got.at[t, pl.ds(0, devices - 1)], sem)

    source = iota((devices, 1), 0)
    cell = iota((devices, full), 1) // wide
    inside = (lane_mod >= 1) & (lane_mod <= wide)

    def finish(t):
        all_sent(t, precv.at[t]).wait()
        for d in range(devices):
            got_rows[d : d + 1] = got[t, d]
        g = got_rows[...]
        before = jnp.where((lane_mod == 0) & (source > 0), g, 0.0)
        after = jnp.where((lane_mod == nc - 1) & (source < devices - 1), g, 0.0)
        before = pltpu.roll(pltpu.roll(before, devices - 1, 0), wide, 1)
        after = pltpu.roll(pltpu.roll(after, 1, 0), LANES - wide, 1)
        g = jnp.where(inside, g, 0.0) + before + after
        high = g.astype(bf16)
        rest = g - high.astype(f32)
        middle = rest.astype(bf16)
        rest = rest - middle.astype(f32)
        d = dot(jnp.concatenate([high, middle, rest.astype(bf16)], axis=0), spread[...])
        d = d[0:devices] + d[devices : 2 * devices] + d[2 * devices : 3 * devices]
        for k in range(kinds):
            row = jnp.sum(jnp.where(cell == source, d[:, k * full : (k + 1) * full], 0.0), axis=0, keepdims=True)
            out_ref[t, k % colours, k // colours : k // colours + 1, :] = row

    blocks = [list(range(frames - 2)), [frames - 2], [frames - 1]]
    for i, times in enumerate(blocks):
        if i == 1:
            pass
        if i == 2:
            pass
        arrive(times)
        if i == 1:
            hear(levels - 1)
        if i:
            send_all(blocks[i - 1])
        for t in times:
            upsample(t)
        for t in times:
            lower(t)
    send_all(blocks[-1])
    for t in range(frames):
        if t == frames - 1:
            pass
        finish(t)

    @pl.when(has_right)
    def _():
        lat_copy(True).wait_send()
        for t in range(frames):
            halo(t, True).wait_send()

    @pl.when(has_left)
    def _():
        lat_copy(False).wait_send()
        for t in range(frames):
            halo(t, False).wait_send()

    for t in range(frames):
        all_sent(t, psend.at[t]).wait()


def per_device(latent, w_in, gain_one, w_mid, gain_two, w_up, gain_three, w_low, gain_four, w_out):
    frames, height, cw, c0 = latent.shape
    devices = lax.axis_size("row")
    assert height == devices
    c1, c2, c3 = w_in.shape[-1], w_up.shape[-1], w_low.shape[-1]
    colours = w_out.shape[-1]
    ext, wide = cw + 2, 2 * cw
    full = wide * devices
    kinds = 2 * colours
    levels = max(1, (devices - 1).bit_length())
    assert 2 * frames * c0 == LANES and kinds * (wide + 2) <= LANES
    packed = cw % 8 != 0
    if packed:
        lat = jnp.transpose(latent, (2, 1, 0, 3)).reshape(cw, height, frames * c0)
        lat = jnp.concatenate([lat, lat], axis=-1)
    else:
        lat = latent
    wup = jnp.transpose(w_up, (0, 1, 3, 2))
    wout = jnp.transpose(w_out, (0, 1, 2, 4, 3))
    tap_rows = -(-9 * colours // 16) * 16

    vmem = pl.BlockSpec(memory_space=pltpu.VMEM)
    hbm = pl.BlockSpec(memory_space=pltpu.HBM)
    dma = pltpu.SemaphoreType.DMA
    return pl.pallas_call(
        functools.partial(kernel, (frames, height, cw, c0, c1, c2, c3, colours), devices, packed),
        out_shape=pltpu.VMEM((frames, colours, 2, full), f32),
        in_specs=[hbm] * 10,
        out_specs=vmem,
        scratch_shapes=[
            pltpu.VMEM((c1 // LANES, LANES), f32),
            pltpu.VMEM((c1 // LANES, LANES), f32),
            pltpu.VMEM((1, c2), f32),
            pltpu.VMEM((1, c3), f32),
            pltpu.VMEM(latent.shape, bf16),
            pltpu.VMEM((height * cw, LANES), f32),
            pltpu.VMEM(w_in.shape, bf16),
            pltpu.VMEM(wup.shape, bf16),
            pltpu.VMEM(w_low.shape, bf16),
            pltpu.VMEM(wout.shape, bf16),
            pltpu.VMEM((3 * 2 * LANES, frames * c1), bf16),
            pltpu.VMEM((3, 3, c1, 3 * c1), bf16),
            pltpu.VMEM((2, 4 * c2, 2 * c1), bf16),
            pltpu.VMEM((2, 2 * c1, 4 * c2), bf16),
            pltpu.VMEM((3, 12 * c2, 2 * LANES), bf16),
            pltpu.VMEM((3, tap_rows, LANES), f32),
            pltpu.VMEM((3, 2 * LANES, 6 * LANES), bf16),
            pltpu.VMEM((LANES, kinds * full), bf16),
            pltpu.VMEM((1, 2 * c2), f32),
            pltpu.VMEM((1, LANES), f32),
            pltpu.VMEM((cw + 4, height, LANES), bf16),
            pltpu.VMEM((cw + 4, height, 2 * LANES), bf16),
            pltpu.VMEM((frames, cw * height, c1), f32),
            pltpu.VMEM((frames, ext, height, 3 * c1), bf16),
            pltpu.VMEM((frames, ext, height, c1), bf16),
            pltpu.VMEM((frames, ext, height, c1), bf16),
            pltpu.VMEM((frames, cw + 1, 2, height, 4 * c2), bf16),
            pltpu.VMEM((frames, wide * height, 2 * LANES), bf16),
            pltpu.VMEM((frames, devices, 1, LANES), f32),
            pltpu.VMEM((frames, devices, 1, LANES), f32),
            pltpu.VMEM((devices, LANES), f32),
            dma((18,)), pltpu.SemaphoreType.REGULAR((2, levels)), dma((2,)), dma((2,)), dma((2, frames)), dma((2, frames)), dma((frames,)), dma((frames,)),
        ],
        compiler_params=pltpu.CompilerParams(
            collective_id=0, has_side_effects=True, vmem_limit_bytes=57 * 1024 * 1024
        ),
    )(
        lat, gain_one.reshape(-1, LANES), gain_two.reshape(-1, LANES), gain_three.reshape(1, c2), gain_four.reshape(1, c3),
        w_in, w_mid, wup, w_low, wout,
    )


def solution(mesh):
    placed = (P("groups", None, "row", None), P(), P(), P(), P(), P(), P(), P(), P(), P())
    return jax.shard_map(
        per_device,
        mesh=mesh,
        in_specs=placed,
        out_specs=P("groups", None, "row", None),
        check_vma=False,
    )
```

```python
import functools

import jax
import jax.numpy as jnp
from jax import lax
from jax.experimental import pallas as pl
from jax.experimental.pallas import tpu as pltpu
from jax.sharding import PartitionSpec as P

eps = 1e-06
f32, bf16, i32 = jnp.float32, jnp.bfloat16, jnp.int32
MESH = pl.DeviceIdType.MESH
LANES = 128


def half_silu(h):
    return h * jnp.tanh(h) + h


def rms_act(field, half_gain, count):
    mean = jnp.sum(field * field, axis=-1, keepdims=True) * (1.0 / count)
    return half_silu(field * lax.rsqrt(mean + eps) * half_gain)


def pair_norm(field, half_gain, low):
    half = field.shape[-1] // 2
    square = field * field
    first = jnp.sum(jnp.where(low, square, 0.0), axis=-1, keepdims=True)
    second = jnp.sum(jnp.where(low, 0.0, square), axis=-1, keepdims=True)
    inv = 1.0 / half
    scale = jnp.where(low, lax.rsqrt(first * inv + eps), lax.rsqrt(second * inv + eps))
    return half_silu(field * scale * half_gain)


def dot(a, b):
    return jnp.dot(a, b, preferred_element_type=f32)


def iota(shape, axis):
    return lax.broadcasted_iota(i32, shape, axis)


def merge(value):
    return value.reshape(-1, value.shape[-1])


def rows_of(value, count):
    return value.reshape(count, value.shape[0] // count, value.shape[1])


def kernel(
    sizes, devices, packed,
    lat_hbm, g1_hbm, g2_hbm, g3_hbm, g4_hbm,
    win_hbm, wmid_hbm, wup_hbm, wlow_hbm, wout_hbm,
    out_ref,
    g1_ref, g2_ref, g3_ref, g4_ref, raw_lat, lat_t, raw_in, raw_up, raw_low, raw_out,
    win, wmid, wupt, wup, wlow, wout_rows, wo, spread, g3x, g4x,
    latx, xs, first, a1, b1, b0, a3, act4, part, got, got_rows,
    wsem, known, lsend, lrecv, hsend, hrecv, psend, precv,
):
    frames, height, cw, c0, c1, c2, c3, colours = sizes
    ext = cw + 2
    wide = 2 * cw
    nc = wide + 2
    fc = frames * c0
    kinds = 2 * colours
    me = lax.axis_index("row")
    is_first, is_last = me == 0, me == devices - 1
    has_left, has_right = me > 0, me < devices - 1

    copies = {}

    def load(name, src, dst, k):
        copies[name] = pltpu.make_async_copy(src, dst, wsem.at[k])
        copies[name].start()

    load("lat", lat_hbm, latx.at[pl.ds(2, cw)] if packed else raw_lat, 0)
    load("in", win_hbm, raw_in, 1)
    gain_refs = [(g1_hbm, g1_ref), (g2_hbm, g2_ref), (g3_hbm, g3_ref), (g4_hbm, g4_ref)]
    for i, (src, dst) in enumerate(gain_refs):
        load(("gain", i), src, dst, 14 + i)
    load("out", wout_hbm, raw_out, 2)
    load("low", wlow_hbm, raw_low, 4)
    for a in range(3):
        for b in range(3):
            load(("mid", a, b), wmid_hbm.at[a, b], wmid.at[:, b, :, pl.ds(a * c1, c1)], 5 + 3 * a + b)
    load("up", wup_hbm, raw_up, 3)

    barrier = pltpu.get_barrier_semaphore()

    for peer, there in ((me - 1, has_left), (me + 1, has_right)):
        @pl.when(there)
        def _(peer=peer):
            pl.semaphore_signal(barrier, inc=1, device_id={"row": peer}, device_id_type=MESH)

    def tell(level):
        step = 2**level
        for side, peer in ((0, me - step), (1, me + step)):
            @pl.when((peer >= 0) & (peer < devices))
            def _(side=side, peer=peer):
                pl.semaphore_signal(known.at[side, level], inc=1, device_id={"row": peer}, device_id_type=MESH)

    def hear(level):
        step = 2**level
        for side, peer in ((1, me - step), (0, me + step)):
            @pl.when((peer >= 0) & (peer < devices))
            def _(side=side):
                pl.semaphore_wait(known.at[side, level], 1)

    levels = known.shape[1]

    copies["lat"].wait()
    if not packed:
        chan, lane = iota((c0, LANES), 0), iota((c0, LANES), 1)
        total = None
        for t in range(frames):
            put = ((lane == t * c0 + chan) | (lane == fc + t * c0 + chan)).astype(bf16)
            field = raw_lat[t].astype(f32).reshape(height * cw, c0).astype(bf16)
            d = dot(field, put)
            total = d if total is None else total + d
        lat_t[...] = total
        for j in range(cw):
            latx[2 + j] = lat_t[pl.ds(j, height, stride=cw), :].astype(bf16)

    pl.semaphore_wait(barrier, has_left.astype(i32) + has_right.astype(i32))

    def lat_copy(right):
        peer = me + 1 if right else me - 1
        src = latx.at[pl.ds(cw, 2)] if right else latx.at[pl.ds(2, 2)]
        dst = latx.at[pl.ds(0, 2)] if right else latx.at[pl.ds(cw + 2, 2)]
        return pltpu.make_async_remote_copy(
            src_ref=src, dst_ref=dst, send_sem=lsend.at[int(right)], recv_sem=lrecv.at[int(right)],
            device_id={"row": peer}, device_id_type=MESH,
        )

    @pl.when(has_right)
    def _():
        lat_copy(True).start()

    @pl.when(has_left)
    def _():
        lat_copy(False).start()

    tell(0)

    @pl.when(is_first)
    def _():
        latx[0:2] = jnp.zeros((2, height, LANES), bf16)
        for t in range(frames):
            b1[t, 0] = jnp.zeros((height, c1), bf16)

    @pl.when(is_last)
    def _():
        latx[cw + 2 : cw + 4] = jnp.zeros((2, height, LANES), bf16)
        for t in range(frames):
            b1[t, ext - 1] = jnp.zeros((height, c1), bf16)

    copies["in"].wait()
    kx = 2 * LANES
    for e in range(3):
        for b in range(3):
            for s in range(frames):
                at = e * kx + b * fc + s * c0
                for t in range(frames):
                    a = s - t + 2
                    block = raw_in[a, b, e] if 0 <= a <= 2 else jnp.zeros((c0, c1), bf16)
                    win[at : at + c0, t * c1 : (t + 1) * c1] = block
        win[e * kx + 3 * fc : (e + 1) * kx, :] = jnp.zeros((kx - 3 * fc, frames * c1), bf16)

    for i in range(4):
        copies[("gain", i)].wait()

    def gain(ref):
        rows = ref[...] * 0.5
        return jnp.concatenate([rows[i : i + 1] for i in range(rows.shape[0])], axis=-1)

    hg1, hg2 = gain(g1_ref), gain(g2_ref)
    g3x[0:1, 0:c2] = g3_ref[...] * 0.5
    g3x[0:1, c2 : 2 * c2] = g3_ref[...] * 0.5
    g4x[...] = jnp.zeros(g4x.shape, f32)
    g4x[0:1, 0:c3] = g4_ref[...] * 0.5

    copies["low"].wait()
    for a in range(3):
        wlow[a] = jnp.zeros(wlow.shape[1:], bf16)
        for e in range(3):
            for b in range(3):
                block = raw_low[a, b, e]
                for q in range(2):
                    at = (4 * e + q + b) * c2
                    wlow[a, at : at + c2, q * LANES : q * LANES + c3] = block

    copies["out"].wait()
    tap_rows = wout_rows.shape[1]
    wout_rows[...] = jnp.zeros(wout_rows.shape, f32)
    for a in range(3):
        for b in range(3):
            for e in range(3):
                at = (3 * b + e) * colours
                wout_rows[a, at : at + colours, 0:c3] = raw_out[a, b, e].astype(f32)
    lane = iota((1, 6 * LANES), 1)
    tap_col = lane // (2 * LANES)
    group = (lane // LANES) % 2
    spot = lane % LANES
    kind = spot // nc
    row_kind, colour = kind // colours, kind % colours
    slot = jnp.where(group == 0, 1 + row_kind, 3 - 3 * row_kind)
    tap = iota((tap_rows, 6 * LANES), 0)
    for q in range(2):
        b = q - slot + 2
        wanted = jnp.where((b >= 0) & (b <= 2) & (kind < kinds), (3 * b + tap_col) * colours + colour, -1)
        select = (tap == wanted).astype(bf16)
        for a in range(3):
            wo[a, q * LANES : (q + 1) * LANES, :] = lax.dot_general(
                wout_rows[a].astype(bf16), select, (((0,), (0,)), ((), ())), preferred_element_type=f32
            ).astype(bf16)

    full = wide * devices
    spot = iota((LANES, full), 0)
    col = iota((LANES, full), 1) % wide
    for k in range(kinds):
        spread[:, k * full : (k + 1) * full] = (spot == k * nc + 1 + col).astype(bf16)

    if 1 < levels:
        hear(0)
        tell(1)

    h3 = iota((1, height, 1), 1)
    top3, bottom3 = h3 == 0, h3 == height - 1
    low_lanes = iota((1, 1, LANES), 2) < fc
    keep_left, keep_right = has_left.astype(f32), has_right.astype(f32)

    def shift_rows(value):
        up = jnp.where(top3, 0.0, pltpu.roll(value, 1, 1))
        down = jnp.where(bottom3, 0.0, pltpu.roll(value, height - 1, 1))
        return up, down

    def stack_rows(j, n):
        v = latx[j : j + n].astype(f32)
        up, down = shift_rows(v)
        xs[j : j + n, :, 0:LANES] = jnp.where(low_lanes, up, v).astype(bf16)
        xs[j : j + n, :, LANES:kx] = jnp.where(low_lanes, down, 0.0).astype(bf16)

    def first_conv(spans, keep):
        lhs = jnp.concatenate(
            [merge(jnp.concatenate([xs[j + e : j + e + n] for j, n in spans], axis=0)) for e in range(3)], axis=-1
        )
        for t in range(frames):
            total = dot(lhs, win[:, t * c1 : (t + 1) * c1])
            act = rms_act(total, hg1, c1)
            if keep is not None:
                act = act * keep
            act = rows_of(act, act.shape[0] // height)
            up, down = shift_rows(act)
            at = 0
            for j, n in spans:
                for c in range(max(j, 1), min(j + n, cw + 1)):
                    first[t, (c - 1) * height : c * height] = total[(at + c - j) * height : (at + c - j + 1) * height]
                for k, value in enumerate((up, act, down)):
                    a1[t, j : j + n, :, k * c1 : (k + 1) * c1] = value[at : at + n].astype(bf16)
                at += n

    stack_rows(2, cw)
    if cw > 2:
        first_conv([(2, cw - 2)], None)

    @pl.when(has_left)
    def _():
        lat_copy(True).wait_recv()

    @pl.when(has_right)
    def _():
        lat_copy(False).wait_recv()

    stack_rows(0, 2)
    stack_rows(cw + 2, 2)
    place = iota((4 * height, 1), 0)
    keep = jnp.where(place < height, keep_left, jnp.where(place >= 3 * height, keep_right, 1.0))
    first_conv([(0, 2), (ext - 2, 2)], keep)

    if 2 < levels:
        hear(1)
        tell(2)

    for a in range(3):
        for b in range(3):
            copies[("mid", a, b)].wait()

    def halo(t, right):
        peer = me + 1 if right else me - 1
        return pltpu.make_async_remote_copy(
            src_ref=b1.at[t, cw if right else 1], dst_ref=b1.at[t, 0 if right else ext - 1],
            send_sem=hsend.at[int(right), t], recv_sem=hrecv.at[int(right), t],
            device_id={"row": peer}, device_id_type=MESH,
        )

    def mix_up():
        for row_odd in range(2):
            for in_row in range(2):
                mixed = []
                for e in range(3):
                    if row_odd == 0:
                        taps = (0, 1) if in_row == 0 else (2,)
                    else:
                        taps = (0,) if in_row == 0 else (1, 2)
                    value = raw_up[taps[0], e].astype(f32)
                    for b in taps[1:]:
                        value = value + raw_up[b, e].astype(f32)
                    mixed.append(value)
                k0, k1, k2 = mixed
                for parity in range(2):
                    pair = (k0 + k1, k2) if parity == 0 else (k0, k1 + k2)
                    at = parity * 2 * c2 + row_odd * c2
                    for in_col in range(2):
                        wupt[in_row, at : at + c2, in_col * c1 : (in_col + 1) * c1] = pair[in_col].astype(bf16)
        for in_row in range(2):
            for i in range(0, 4 * c2, LANES):
                for j in range(0, 2 * c1, LANES):
                    wup[in_row, j : j + LANES, i : i + LANES] = wupt[in_row, i : i + LANES, j : j + LANES].T

    copies["up"].wait()
    sums = {t: [] for t in range(frames)}
    m = cw * height
    tasks = [(0, 1, 2), (1, 2, 2), (0, 0, 0), (1, 0, 1)]
    tasks = [(s, low, high) for s, low, high in tasks if s - high + 2 < frames]
    tasks += [(s, max(0, 3 - frames + s), 2) for s in range(2, frames)]
    assert frames >= 3
    left = {t: min(3, t + 1) for t in range(frames)}
    sent_count = 0
    for s, least, most in tasks:
        least = max(least, 3 - frames + s)
        lhs = jnp.concatenate([merge(a1[s, e : e + cw]) for e in range(3)], axis=-1)
        rhs = merge(wmid[:, :, :, least * c1 : (most + 1) * c1])
        paired = rhs.shape[1] // 512 * 512
        cut = rhs.shape[0] // 512 * 256 + (256 if rhs.shape[0] % 512 else 0)
        d = dot(lhs[:, :cut], rhs[:cut, paired:]) + dot(lhs[:, cut:], rhs[cut:, paired:])
        if paired:
            d = jnp.concatenate([dot(lhs, rhs[:, :paired]), d], axis=-1)
        done = []
        for a in range(least, most + 1):
            t = s - a + 2
            sums[t].append(d[:, (a - least) * c1 : (a - least + 1) * c1])
            left[t] -= 1
            if left[t] == 0:
                done.append(t)
        for t in done:
            total = first[t]
            for v in sums[t]:
                total = total + v
            b1[t, 1 : cw + 1] = rows_of(rms_act(total, hg2, c1).astype(bf16), cw)
            sent_count += 1

        if done and sent_count in (2, frames):
            times = list(range(2)) if sent_count == 2 else list(range(2, frames))

            @pl.when(has_right)
            def _(times=times):
                for t in times:
                    halo(t, True).start()

            @pl.when(has_left)
            def _(times=times):
                for t in times:
                    halo(t, False).start()

            if levels > 3 and sent_count == 2:
                hear(2)
                tell(3)
            if sent_count == 2:
                mix_up()
            if sent_count == frames:
                for level in range(4, levels):
                    hear(level - 1)
                    tell(level)

    low3 = iota((1, 2 * c2), 1) < c2
    pairs = cw + 1
    tall = iota((pairs * height, 1), 0)
    top = tall % height == 0
    bottom = tall % height == height - 1
    hg3, hg4 = g3x[...], g4x[...]

    def arrive(times):
        @pl.when(has_left)
        def _():
            for t in times:
                halo(t, True).wait_recv()

        @pl.when(has_right)
        def _():
            for t in times:
                halo(t, False).wait_recv()

    def upsample(t):
        b0[t] = pltpu.roll(b1[t].astype(f32), 1, 1).astype(bf16)
        above = jnp.concatenate([merge(b0[t, e : e + pairs]) for e in range(2)], axis=-1)
        here = jnp.concatenate([merge(b1[t, e : e + pairs]) for e in range(2)], axis=-1)
        from_above, from_here = dot(above, wup[0]), dot(here, wup[1])
        for parity in range(2):
            span = slice(parity * 2 * c2, (parity + 1) * 2 * c2)
            field = jnp.where(top & ~low3, 0.0, from_above[:, span]) + jnp.where(top & low3, 0.0, from_here[:, span])
            act = pair_norm(field, hg3, low3)
            if parity == 0:
                act = act * jnp.where(tall < height, keep_left, 1.0)
            else:
                act = act * jnp.where(tall >= cw * height, keep_right, 1.0)
            act = rows_of(act, pairs)
            ahead = pltpu.roll(act, height - 1, 1)
            low = low3.reshape(1, 1, 2 * c2)
            a3[t, :, parity, :, 0 : 2 * c2] = jnp.where(top3 & low, 0.0, act).astype(bf16)
            a3[t, :, parity, :, 2 * c2 : 4 * c2] = jnp.where(bottom3 & ~low, 0.0, ahead).astype(bf16)

    lane_mod = iota((1, LANES), 1) % nc
    h2 = iota((height, 1), 0)
    even_kind = iota((1, LANES), 1) < colours * nc

    def message(t):
        def copy(k, act):
            peer = lax.rem(me + k, devices)
            return pltpu.make_async_remote_copy(
                src_ref=part.at[t, peer], dst_ref=got.at[t, me], send_sem=psend.at[t], recv_sem=precv.at[t],
                device_id={"row": peer}, device_id_type=MESH,
            )
        return copy

    def lower(t):
        half = wide // 2 * height
        for i in range(2):
            total = None
            for a in range(3):
                s = t + a - 2
                if s < 0:
                    continue
                field = a3[s].reshape(nc, height, 4 * c2)
                c = i * wide // 2
                lhs = jnp.concatenate([merge(field[c + e : c + e + wide // 2]) for e in range(3)], axis=-1)
                d = dot(lhs, wlow[a])
                total = d if total is None else total + d
            for q in range(2):
                span = slice(q * LANES, (q + 1) * LANES)
                act4[t, i * half : (i + 1) * half, span] = rms_act(total[:, span], hg4, c3).astype(bf16)
        main, rest = None, [None, None]
        for a in range(3):
            s = t + a - 2
            if s < 0:
                continue
            d = dot(act4[s], wo[a, :, : 4 * LANES])
            main = d if main is None else main + d
            for i in range(2):
                d = dot(act4[s, i * half : (i + 1) * half], wo[a, :, 4 * LANES :])
                rest[i] = d if rest[i] is None else rest[i] + d
        total = jnp.concatenate([main, jnp.concatenate(rest, axis=0)], axis=-1)
        out = [None, None]
        for e in range(3):
            for c in range(wide):
                for g in range(2):
                    at = (2 * e + g) * LANES
                    v = jnp.where(lane_mod == c + 2 - e, total[c * height : (c + 1) * height, at : at + LANES], 0.0)
                    out[g] = v if out[g] is None else out[g] + v
        down = jnp.where(h2 == 0, 0.0, pltpu.roll(out[1], 1, 0))
        up = jnp.where(h2 == height - 1, 0.0, pltpu.roll(out[1], height - 1, 0))
        value = out[0] + jnp.where(even_kind, down, up)
        for d in range(devices):
            part[t, d] = value[d : d + 1]
        got[t, me] = part[t, me]

    def send_all(times):
        def send(k, _):
            for t in times:
                message(t)(k, None).start()
            return _

        lax.fori_loop(1, devices, send, 0)

    def all_sent(t, sem):
        return pltpu.make_async_copy(got.at[t, pl.ds(0, devices - 1)], got.at[t, pl.ds(0, devices - 1)], sem)

    source = iota((devices, 1), 0)
    cell = iota((devices, full), 1) // wide
    inside = (lane_mod >= 1) & (lane_mod <= wide)

    def finish(t):
        all_sent(t, precv.at[t]).wait()
        for d in range(devices):
            got_rows[d : d + 1] = got[t, d]
        g = got_rows[...]
        before = jnp.where((lane_mod == 0) & (source > 0), g, 0.0)
        after = jnp.where((lane_mod == nc - 1) & (source < devices - 1), g, 0.0)
        before = pltpu.roll(pltpu.roll(before, devices - 1, 0), wide, 1)
        after = pltpu.roll(pltpu.roll(after, 1, 0), LANES - wide, 1)
        g = jnp.where(inside, g, 0.0) + before + after
        high = g.astype(bf16)
        rest = g - high.astype(f32)
        middle = rest.astype(bf16)
        rest = rest - middle.astype(f32)
        d = dot(jnp.concatenate([high, middle, rest.astype(bf16)], axis=0), spread[...])
        d = d[0:devices] + d[devices : 2 * devices] + d[2 * devices : 3 * devices]
        for k in range(kinds):
            row = jnp.sum(jnp.where(cell == source, d[:, k * full : (k + 1) * full], 0.0), axis=0, keepdims=True)
            out_ref[t, k % colours, k // colours : k // colours + 1, :] = row

    blocks = [list(range(frames - 2)), [frames - 2], [frames - 1]]
    for i, times in enumerate(blocks):
        arrive(times)
        if i == 1:
            hear(levels - 1)
        if i:
            send_all(blocks[i - 1])
        for t in times:
            upsample(t)
        for t in times:
            lower(t)
    send_all(blocks[-1])
    for t in range(frames):
        finish(t)

    @pl.when(has_right)
    def _():
        lat_copy(True).wait_send()
        for t in range(frames):
            halo(t, True).wait_send()

    @pl.when(has_left)
    def _():
        lat_copy(False).wait_send()
        for t in range(frames):
            halo(t, False).wait_send()

    for t in range(frames):
        all_sent(t, psend.at[t]).wait()


def per_device(latent, w_in, gain_one, w_mid, gain_two, w_up, gain_three, w_low, gain_four, w_out):
    frames, height, cw, c0 = latent.shape
    devices = lax.axis_size("row")
    assert height == devices
    c1, c2, c3 = w_in.shape[-1], w_up.shape[-1], w_low.shape[-1]
    colours = w_out.shape[-1]
    ext, wide = cw + 2, 2 * cw
    full = wide * devices
    kinds = 2 * colours
    levels = max(1, (devices - 1).bit_length())
    assert 2 * frames * c0 == LANES and kinds * (wide + 2) <= LANES
    packed = cw % 8 != 0
    if packed:
        lat = jnp.transpose(latent, (2, 1, 0, 3)).reshape(cw, height, frames * c0)
        lat = jnp.concatenate([lat, lat], axis=-1)
    else:
        lat = latent
    wup = jnp.transpose(w_up, (0, 1, 3, 2))
    wout = jnp.transpose(w_out, (0, 1, 2, 4, 3))
    tap_rows = -(-9 * colours // 16) * 16

    vmem = pl.BlockSpec(memory_space=pltpu.VMEM)
    hbm = pl.BlockSpec(memory_space=pltpu.HBM)
    dma = pltpu.SemaphoreType.DMA
    return pl.pallas_call(
        functools.partial(kernel, (frames, height, cw, c0, c1, c2, c3, colours), devices, packed),
        out_shape=pltpu.VMEM((frames, colours, 2, full), f32),
        in_specs=[hbm] * 10,
        out_specs=vmem,
        scratch_shapes=[
            pltpu.VMEM((c1 // LANES, LANES), f32),
            pltpu.VMEM((c1 // LANES, LANES), f32),
            pltpu.VMEM((1, c2), f32),
            pltpu.VMEM((1, c3), f32),
            pltpu.VMEM(latent.shape, bf16),
            pltpu.VMEM((height * cw, LANES), f32),
            pltpu.VMEM(w_in.shape, bf16),
            pltpu.VMEM(wup.shape, bf16),
            pltpu.VMEM(w_low.shape, bf16),
            pltpu.VMEM(wout.shape, bf16),
            pltpu.VMEM((3 * 2 * LANES, frames * c1), bf16),
            pltpu.VMEM((3, 3, c1, 3 * c1), bf16),
            pltpu.VMEM((2, 4 * c2, 2 * c1), bf16),
            pltpu.VMEM((2, 2 * c1, 4 * c2), bf16),
            pltpu.VMEM((3, 12 * c2, 2 * LANES), bf16),
            pltpu.VMEM((3, tap_rows, LANES), f32),
            pltpu.VMEM((3, 2 * LANES, 6 * LANES), bf16),
            pltpu.VMEM((LANES, kinds * full), bf16),
            pltpu.VMEM((1, 2 * c2), f32),
            pltpu.VMEM((1, LANES), f32),
            pltpu.VMEM((cw + 4, height, LANES), bf16),
            pltpu.VMEM((cw + 4, height, 2 * LANES), bf16),
            pltpu.VMEM((frames, cw * height, c1), f32),
            pltpu.VMEM((frames, ext, height, 3 * c1), bf16),
            pltpu.VMEM((frames, ext, height, c1), bf16),
            pltpu.VMEM((frames, ext, height, c1), bf16),
            pltpu.VMEM((frames, cw + 1, 2, height, 4 * c2), bf16),
            pltpu.VMEM((frames, wide * height, 2 * LANES), bf16),
            pltpu.VMEM((frames, devices, 1, LANES), f32),
            pltpu.VMEM((frames, devices, 1, LANES), f32),
            pltpu.VMEM((devices, LANES), f32),
            dma((18,)), pltpu.SemaphoreType.REGULAR((2, levels)), dma((2,)), dma((2,)), dma((2, frames)), dma((2, frames)), dma((frames,)), dma((frames,)),
        ],
        compiler_params=pltpu.CompilerParams(
            collective_id=0, has_side_effects=True, vmem_limit_bytes=57 * 1024 * 1024
        ),
    )(
        lat, gain_one.reshape(-1, LANES), gain_two.reshape(-1, LANES), gain_three.reshape(1, c2), gain_four.reshape(1, c3),
        w_in, w_mid, wup, w_low, wout,
    )


def solution(mesh):
    placed = (P("groups", None, "row", None), P(), P(), P(), P(), P(), P(), P(), P(), P())
    return jax.shard_map(
        per_device,
        mesh=mesh,
        in_specs=placed,
        out_specs=P("groups", None, "row", None),
        check_vma=False,
    )
```
